256 devices in a mesh: node: 2 (over y_lo), space: 128 (over y_hi, x, z, core).
Axes of the slice: x: 4, y: 4 (y_hi: 2, y_lo: 2; y = y_hi * 2 + y_lo), z: 8, core: 2. Of those that a mesh axis runs over, the one named last changes fastest.
Arguments:
- u_start: float32 [1024, 256, 128], P('space'), may hold values from 0 to 1
- v_start: float32 [1024, 256, 128], P('space'), may hold values from 0 to 2
- labels: int32 [1024, 256, 128], P('space'), may hold values from 0 to 2
- u_guess: float32 [4, 1024, 256, 128], P('node', 'space'), may hold values from 0 to 1
- v_guess: float32 [4, 1024, 256, 128], P('node', 'space'), may hold values from 0 to 2
Outputs:
- u_nodes: float32 [4, 1024, 256, 128], P('node', 'space')
- v_nodes: float32 [4, 1024, 256, 128], P('node', 'space')
The draws below stay inside these ranges and needn't reach their ends.
Inputs may be any that keep to these rules, and one draw needn't show every extreme that they name: `labels`: 0 marks healthy, 1 fibrous and 2 scar tissue.
All inputs are finite; a program needn't handle non-finite values.
Results may differ from the reference program's by a relative error of at most 0.0001.
Values sent between devices are 32-bit elements; how exact they have to be, the bound alone decides.
A program may use at most 192 MiB of HBM per device.

```python
import jax
import jax.numpy as jnp
from jax import lax

NY = 256
NZ = 128
NODES = 4
SWEEPS = 2
NX = 1024


def set_ends(result, rng, smallest, largest):
    longest = result.shape.index(max(result.shape))
    spots = []
    for shift in (0, 1):
        where = [jax.random.randint(jax.random.fold_in(rng, axis), (), 0, length) for axis, length in enumerate(result.shape)]
        where[longest] = (where[longest] + shift) % result.shape[longest]
        spots.append(tuple(where))
    return result.at[spots[0]].set(smallest).at[spots[1]].set(largest)


def levels(own_key, shape, split, smallest, top_value):
    def one(dim, shards_of):
        heights = jax.random.uniform(jax.random.fold_in(jax.random.fold_in(own_key, 6), dim), (shards_of,), jnp.float32, smallest / len(split), top_value / len(split))
        return jnp.repeat(jnp.exp(heights), shape[dim] // shards_of).reshape((-1,) + (1,) * (len(shape) - dim - 1))

    gain = one(*split[0])
    for cut in split[1:]:
        gain = gain * one(*cut)
    return gain


def setup_inputs(seed: int = 0) -> dict:
    seeds = jax.random.split(jax.random.key(seed), 6)
    return {
        "u_start": jnp.clip(1.0 * jax.random.uniform(seeds[0], (NX, NY, NZ), jnp.float32) ** levels(seeds[0], (NX, NY, NZ), ((0, 128),), -0.2, 0.2), 0.0, 1.0),
        "v_start": jnp.clip(2.0 * jax.random.uniform(seeds[1], (NX, NY, NZ), jnp.float32) ** levels(seeds[1], (NX, NY, NZ), ((0, 128),), -0.2, 0.2), 0.0, 2.0),
        "labels": set_ends(jax.random.randint(seeds[2], (NX, NY, NZ), 0, 3), jax.random.fold_in(seeds[2], 1), 0, 2).astype(jnp.int32),
        "u_guess": jnp.clip(1.0 * jax.random.uniform(seeds[3], (NODES, NX, NY, NZ), jnp.float32) ** levels(seeds[3], (NODES, NX, NY, NZ), ((0, 2), (1, 128)), -0.2, 0.2), 0.0, 1.0),
        "v_guess": jnp.clip(2.0 * jax.random.uniform(seeds[4], (NODES, NX, NY, NZ), jnp.float32) ** levels(seeds[4], (NODES, NX, NY, NZ), ((0, 2), (1, 128)), -0.2, 0.2), 0.0, 2.0),
    }


radau_points = (0.08858795951270395, 0.4094668644407347, 0.7876594617608471, 1.0)
time_step = 0.16
onset_level = 0.15
ionic_gain = 8.0
recovery_base = 0.002
recovery_slope = 0.2
recovery_offset = 0.3
conductances = (1.0, 0.35, 0.05)
excitability = (1.0, 0.6, 0.0)


def weight_table():
    table = []
    for target in range(4):
        entries = []
        for column in range(4):
            coeffs = [1.0]
            for other in range(4):
                if other != column:
                    factor = 1.0 / (radau_points[column] - radau_points[other])
                    raised = [0.0] + coeffs
                    lowered = coeffs + [0.0]
                    coeffs = [factor * (raised[place] - radau_points[other] * lowered[place]) for place in range(len(raised))]
            integral = 0.0
            for place in range(len(coeffs)):
                integral = integral + coeffs[place] * radau_points[target] ** (place + 1) / (place + 1)
            entries.append(time_step * integral)
        table.append(entries)
    return table


def label_values(labels, values):
    return jnp.where(labels == 0, jnp.float32(values[0]),
                     jnp.where(labels == 1, jnp.float32(values[1]), jnp.float32(values[2])))


def neighbours(field):
    padded = jnp.pad(field, 1)
    return (padded[2:, 1:-1, 1:-1], padded[:-2, 1:-1, 1:-1],
            padded[1:-1, 2:, 1:-1], padded[1:-1, :-2, 1:-1],
            padded[1:-1, 1:-1, 2:], padded[1:-1, 1:-1, :-2])


def rates(u_field, v_field, conduct, excite):
    conduct_sides = neighbours(conduct)
    voltage_sides = neighbours(u_field)
    spread = jnp.zeros_like(u_field)
    for conduct_side, voltage_side in zip(conduct_sides, voltage_sides):
        facing = 2.0 * conduct * conduct_side / (conduct + conduct_side)
        spread = spread + facing * (voltage_side - u_field)
    ionic = ionic_gain * u_field * (u_field - onset_level) * (1.0 - u_field) - u_field * v_field
    rate_u = spread + excite * ionic
    recovery = recovery_base + recovery_slope * v_field / jnp.maximum(u_field + recovery_offset, recovery_offset)
    rate_v = recovery * (-v_field - ionic_gain * u_field * (u_field - onset_level - 1.0))
    return rate_u, rate_v


def reference(u_start, v_start, labels, u_guess, v_guess):
    conduct = label_values(labels, conductances)
    excite = label_values(labels, excitability)
    weights = jnp.asarray(weight_table(), jnp.float32)
    u_nodes, v_nodes = u_guess, v_guess
    for sweep_index in range(SWEEPS):
        rate_u, rate_v = lax.map(lambda node_pair: rates(node_pair[0], node_pair[1], conduct, excite), (u_nodes, v_nodes))
        u_nodes = u_start[None] + jnp.einsum("ij,jabc->iabc", weights, rate_u, precision=lax.Precision.HIGHEST)
        v_nodes = v_start[None] + jnp.einsum("ij,jabc->iabc", weights, rate_v, precision=lax.Precision.HIGHEST)
    return u_nodes, v_nodes
```

```python
import jax
import jax.numpy as jnp
from jax import lax
from jax.experimental import pallas as pl
from jax.experimental.pallas import tpu as pltpu
from jax.sharding import PartitionSpec as P

MESH = pl.DeviceIdType.MESH
LANES = 128
CHUNK = 16
EDGE = 8
LAG = 2

radau_points = (0.08858795951270396, 0.4094668644407347, 0.7876594617608471, 1.0)
time_step = 0.16
onset_level = 0.15
ionic_gain = 8.0
recovery_base = 0.002
recovery_slope = 0.2
recovery_offset = 0.3
conductances = (1.0, 0.35, 0.05)
excitability = (1.0, 0.6, 0.0)


def weight_table():
    table = []
    for target in range(4):
        entries = []
        for column in range(4):
            coeffs = [1.0]
            for other in range(4):
                if other != column:
                    factor = 1.0 / (radau_points[column] - radau_points[other])
                    raised = [0.0] + coeffs
                    lowered = coeffs + [0.0]
                    coeffs = [
                        factor * (raised[place] - radau_points[other] * lowered[place])
                        for place in range(len(raised))
                    ]
            integral = 0.0
            for place in range(len(coeffs)):
                integral = integral + coeffs[place] * radau_points[target] ** (place + 1) / (
                    place + 1
                )
            entries.append(time_step * integral)
        table.append(entries)
    return table


def label_values(labels, values, outside):
    return jnp.where(
        labels == 0,
        jnp.float32(values[0]),
        jnp.where(
            labels == 1,
            jnp.float32(values[1]),
            jnp.where(labels == 2, jnp.float32(values[2]), jnp.float32(outside)),
        ),
    )


def kernel(
    us_hbm,
    vs_hbm,
    lab_hbm,
    ug_hbm,
    vg_hbm,
    out_u,
    out_v,
    u0,
    u1,
    v,
    res,
    us,
    vs,
    lab,
    cond,
    face,
    exc,
    b0s,
    b0r,
    b1s,
    b1r,
    load_sem,
    lab_send,
    lab_recv,
    own_send,
    own_recv,
    fwd_send,
    fwd_recv,
    mid_send,
    mid_recv,
    row_send,
    row_recv,
    in_send,
    in_recv,
    back_send,
    back_recv,
):
    depth, rows = lab_hbm.shape[0], lab_hbm.shape[1] // 2
    chunks = rows // CHUNK
    node, here = lax.axis_index("node"), lax.axis_index("space")
    count = lax.axis_size("space")
    fold = count // 2
    half = lax.rem(node + here // fold, 2)
    own, other = half * rows, (1 - half) * rows
    has = (here > 0, here < count - 1)
    flips = ((here == fold).astype(jnp.int32), (here == fold - 1).astype(jnp.int32))
    sides = (
        (lax.rem(node + flips[0], 2), here - 1),
        (lax.rem(node + flips[1], 2), here + 1),
    )
    partner = (1 - node, here)
    ours = (1, depth)
    theirs = (depth + 1, 0)

    def mine(k):
        return k * half + (chunks - 1 - k) * (1 - half)

    def its(k):
        return k * (1 - half) + (chunks - 1 - k) * half

    def rows_of(c, base):
        return pl.ds(pl.multiple_of(base + CHUNK * c, 8), CHUNK)

    def remote(src, dst, send, recv, device):
        return pltpu.make_async_remote_copy(
            src_ref=src,
            dst_ref=dst,
            send_sem=send,
            recv_sem=recv,
            device_id=device,
            device_id_type=MESH,
        )

    own_rows = pl.ds(pl.multiple_of(own, 8), rows)
    inner = pl.ds(EDGE, rows)
    slab = pl.ds(1, depth)
    edge_source = pl.ds(pl.multiple_of(rows - EDGE * half, 8), EDGE)
    edge_place = pl.ds(pl.multiple_of((EDGE + rows) * (1 - half), 8), EDGE)
    void_place = pl.ds(pl.multiple_of((EDGE + rows) * half, 8), EDGE)

    def lab_copy(side):
        return remote(
            lab_hbm.at[pl.ds(ours[side] - 1, 1), own_rows],
            lab.at[pl.ds(theirs[side], 1), inner],
            lab_send.at[side],
            lab_recv.at[1 - side],
            sides[side],
        )

    def own_copy(side):
        return remote(
            ug_hbm.at[:, pl.ds(ours[side] - 1, 1), own_rows],
            u0.at[pl.ds(2 * flips[side], 2), pl.ds(theirs[side], 1), inner],
            own_send.at[side],
            own_recv.at[1 - side],
            sides[side],
        )

    def fwd_copy(side, k):
        at = rows_of(mine(k), EDGE)
        return remote(
            u0.at[pl.ds(2, 2), pl.ds(ours[side], 1), at],
            u0.at[pl.ds(2 - 2 * flips[side], 2), pl.ds(theirs[side], 1), at],
            fwd_send.at[side, k],
            fwd_recv.at[1 - side, k],
            sides[side],
        )

    def mid_copy(side, pair, k):
        at = rows_of(mine(k), EDGE)
        to = 2 * (pair + flips[side] - 2 * pair * flips[side])
        return remote(
            u1.at[pl.ds(2 * pair, 2), pl.ds(ours[side], 1), at],
            u1.at[pl.ds(to, 2), pl.ds(theirs[side], 1), at],
            mid_send.at[side, pair, k],
            mid_recv.at[1 - side, pair, k],
            sides[side],
        )

    def in_copy(field, k, c, base):
        return remote(
            (ug_hbm, vg_hbm)[field].at[:, :, rows_of(c, base)],
            (
                u0.at[pl.ds(2, 2), slab, rows_of(c, EDGE)],
                v.at[pl.ds(2, 2), :, rows_of(c, 0)],
            )[field],
            in_send.at[field, k],
            in_recv.at[field, k],
            partner,
        )

    def sent(field, k):
        return in_copy(field, k, its(k), other)

    def arriving(field, k):
        return in_copy(field, k, mine(k), own)

    def back_copies(k, base, c):
        return (
            remote(
                res.at[:, :, rows_of(c, 0)],
                out_u.at[:, :, rows_of(c, base)],
                back_send.at[0, k],
                back_recv.at[0, k],
                partner,
            ),
            remote(
                v.at[pl.ds(2, 2), :, rows_of(c, 0)],
                out_v.at[:, :, rows_of(c, base)],
                back_send.at[1, k],
                back_recv.at[1, k],
                partner,
            ),
        )

    row_copies = (
        remote(b0s, b0r, row_send.at[0], row_recv.at[0], partner),
        remote(b1s, b1r, row_send.at[1], row_recv.at[1], partner),
    )

    loads = [
        pltpu.make_async_copy(src, dst, load_sem.at[i])
        for i, (src, dst) in enumerate(
            (
                (ug_hbm.at[:, :, own_rows], u0.at[pl.ds(0, 2), slab, inner]),
                (lab_hbm.at[:, own_rows], lab.at[slab, inner]),
                (lab_hbm.at[:, edge_source], lab.at[slab, edge_place]),
                (ug_hbm.at[:, :, edge_source], u0.at[pl.ds(0, 2), slab, edge_place]),
                (vg_hbm.at[:, :, own_rows], v.at[pl.ds(0, 2)]),
                (us_hbm.at[:, own_rows], us),
                (vs_hbm.at[:, own_rows], vs),
            )
        )
    ]

    barrier = pltpu.get_barrier_semaphore()
    pl.semaphore_signal(barrier, inc=1, device_id=partner, device_id_type=MESH)
    for side in (0, 1):

        @pl.when(has[side])
        def _():
            pl.semaphore_signal(barrier, inc=1, device_id=sides[side], device_id_type=MESH)

    loads[0].start()
    pl.semaphore_wait(barrier, 1 + has[0].astype(jnp.int32) + has[1].astype(jnp.int32))

    for k in (0, 1):
        sent(0, k).start()
    for copy in loads[1:]:
        copy.start()
    for side in (0, 1):

        @pl.when(has[side])
        def _():
            lab_copy(side).start()
            own_copy(side).start()

    def take_row(source, target, nodes):
        @pl.when(half == 0)
        def _():
            for j in range(nodes):
                for p in range(depth):
                    target[j, p : p + 1] = source[j, p + 1, EDGE + rows - 1 : EDGE + rows]

        @pl.when(half == 1)
        def _():
            for j in range(nodes):
                for p in range(depth):
                    target[j, p : p + 1] = source[j, p + 1, EDGE : EDGE + 1]

    def put_row(source, target, nodes, first):
        @pl.when(half == 0)
        def _():
            for j in range(nodes):
                for p in range(depth):
                    target[first(j), p + 1, EDGE + rows : EDGE + rows + 1] = source[j, p : p + 1]

        @pl.when(half == 1)
        def _():
            for j in range(nodes):
                for p in range(depth):
                    target[first(j), p + 1, EDGE - 1 : EDGE] = source[j, p : p + 1]

    loads[0].wait()
    take_row(u0, b0s, 2)
    row_copies[0].start()

    @pl.loop(2, chunks)
    def _(k):
        sent(0, k).start()

    @pl.loop(0, chunks)
    def _(k):
        sent(1, k).start()

    for place in range(4):
        for p in range(depth):
            u0[place, p + 1, void_place] = jnp.zeros((EDGE, LANES), jnp.float32)
            u1[place, p + 1, void_place] = jnp.zeros((EDGE, LANES), jnp.float32)
    for p in range(depth):
        lab[p + 1, void_place] = jnp.full((EDGE, LANES), 3, jnp.int32)
    for side in (0, 1):

        @pl.when(jnp.logical_not(has[side]))
        def _():
            plane = (0, depth + 1)[side]

            @pl.loop(0, chunks)
            def _(c):
                at = rows_of(c, EDGE)
                lab[plane, at] = jnp.full((CHUNK, LANES), 3, jnp.int32)
                for place in range(4):
                    u0[place, plane, at] = jnp.zeros((CHUNK, LANES), jnp.float32)
                    u1[place, plane, at] = jnp.zeros((CHUNK, LANES), jnp.float32)

    loads[1].wait()
    loads[2].wait()
    for side in (0, 1):

        @pl.when(has[side])
        def _():
            lab_copy(1 - side).wait_recv()

    @pl.loop(0, depth + 2)
    def _(p):
        for c in range(chunks):
            at = pl.ds(EDGE + CHUNK * c, CHUNK)
            cond[p, at] = label_values(lab[p, at], conductances, 0.0)

    for p in range(depth):
        for at in (pl.ds(0, EDGE), pl.ds(EDGE + rows, EDGE)):
            cond[p + 1, at] = label_values(lab[p + 1, at], conductances, 0.0)

    lane = lax.broadcasted_iota(jnp.int32, (CHUNK, LANES), 1)

    @pl.loop(0, depth)
    def _(p):
        @pl.loop(0, chunks)
        def _(c):
            at, to = rows_of(c, EDGE), rows_of(c, 0)
            row = EDGE + CHUNK * c
            center = cond[p + 1, at]
            beside = (
                cond[p + 2, at],
                cond[p, at],
                cond[p + 1, pl.ds(row + 1, CHUNK)],
                cond[p + 1, pl.ds(row - 1, CHUNK)],
                jnp.where(lane == LANES - 1, 0.0, pltpu.roll(center, LANES - 1, 1)),
                jnp.where(lane == 0, 0.0, pltpu.roll(center, 1, 1)),
            )
            total = jnp.zeros_like(center)
            for i in range(6):
                value = 2.0 * center * beside[i] / (center + beside[i])
                face[i, p, to] = value
                total = total + value
            face[6, p, to] = total
            exc[p, to] = label_values(lab[p + 1, at], excitability, 0.0)

    for copy in loads[3:]:
        copy.wait()
    row_copies[0].wait_recv()
    put_row(b0r, u0, 2, lambda j: 2 + j)

    @pl.loop(0, chunks)
    def _(k):
        arriving(0, k).wait_recv()
        for side in (0, 1):

            @pl.when(has[side])
            def _():
                fwd_copy(side, k).start()

    for side in (0, 1):

        @pl.when(has[side])
        def _():
            own_copy(1 - side).wait_recv()

    table = weight_table()
    weights = [
        [
            jnp.where(
                node == 0,
                jnp.float32(table[m][j]),
                jnp.float32(table[(m + 2) % 4][(j + 2) % 4]),
            )
            for j in range(4)
        ]
        for m in range(4)
    ]

    def sweep(source, c, write):
        at, to = rows_of(c, EDGE), rows_of(c, 0)
        row = EDGE + CHUNK * c

        @pl.loop(0, depth)
        def _(p):
            faces = [face[i, p, to] for i in range(7)]
            excite = exc[p, to]
            sum_u = [us[p, to]] * 4
            sum_v = [vs[p, to]] * 4
            for j in range(4):
                mid = source[j, p + 1, at]
                v_mid = v[j, p, to]
                spread = (
                    faces[0] * source[j, p + 2, at]
                    + faces[1] * source[j, p, at]
                    + faces[2] * source[j, p + 1, pl.ds(row + 1, CHUNK)]
                    + faces[3] * source[j, p + 1, pl.ds(row - 1, CHUNK)]
                    + faces[4] * pltpu.roll(mid, LANES - 1, 1)
                    + faces[5] * pltpu.roll(mid, 1, 1)
                )
                scaled = ionic_gain * mid
                growth = (scaled - ionic_gain * onset_level) * (1.0 - mid) - v_mid
                rate_u = spread + mid * (excite * growth - faces[6])
                recovery = recovery_base + recovery_slope * v_mid / jnp.maximum(
                    mid + recovery_offset, recovery_offset
                )
                rate_v = recovery * (-v_mid - scaled * (mid - (onset_level + 1.0)))
                for m in range(4):
                    sum_u[m] = sum_u[m] + weights[m][j] * rate_u
                    sum_v[m] = sum_v[m] + weights[m][j] * rate_v
            write(p, sum_u, sum_v)

    def first_sweep(k):
        c = mine(k)
        at, to = rows_of(c, EDGE), rows_of(c, 0)

        def write(p, new_u, new_v):
            for m in range(4):
                u1[m, p + 1, at] = new_u[m]
                v[m, p, to] = new_v[m]

        sweep(u0, c, write)

    def second_sweep(k):
        c = mine(k)
        to, full = rows_of(c, 0), rows_of(c, own)
        for side in (0, 1):

            @pl.when(has[side])
            def _():
                for pair in (0, 1):
                    mid_copy(1 - side, pair, k).wait_recv()

        def write(p, new_u, new_v):
            for m in range(2):
                out_u[m, p, full] = new_u[m]
                out_v[m, p, full] = new_v[m]
                res[m, p, to] = new_u[2 + m]
                v[2 + m, p, to] = new_v[2 + m]

        sweep(u1, c, write)
        for copy in back_copies(k, own, c):
            copy.start()

    @pl.loop(0, chunks)
    def _(k):
        arriving(1, k).wait_recv()
        for side in (0, 1):

            @pl.when(has[side])
            def _():
                fwd_copy(1 - side, k).wait_recv()

        first_sweep(k)
        for side in (0, 1):

            @pl.when(has[side])
            def _():
                for pair in (0, 1):
                    mid_copy(side, pair, k).start()

        @pl.when(k == 0)
        def _():
            take_row(u1, b1s, 4)
            row_copies[1].start()

        @pl.when(k > LAG)
        def _():
            second_sweep(k - LAG)

    @pl.loop(chunks - LAG, chunks)
    def _(k):
        second_sweep(k)

    row_copies[1].wait_recv()
    put_row(b1r, u1, 4, lambda j: (j + 2) % 4)
    second_sweep(0)

    @pl.loop(0, chunks)
    def _(k):
        for field in (0, 1):
            sent(field, k).wait_send()
        for copy in back_copies(k, own, mine(k)):
            copy.wait_send()
        for side in (0, 1):

            @pl.when(has[side])
            def _():
                fwd_copy(side, k).wait_send()
                for pair in (0, 1):
                    mid_copy(side, pair, k).wait_send()

    for copy in row_copies:
        copy.wait_send()
    for side in (0, 1):

        @pl.when(has[side])
        def _():
            lab_copy(side).wait_send()
            own_copy(side).wait_send()

    @pl.loop(0, chunks)
    def _(k):
        for copy in back_copies(k, other, its(k)):
            copy.wait_recv()


def on_device(*arguments):
    labels = arguments[2]
    depth, width = labels.shape[0], labels.shape[1]
    rows = width // 2
    chunks = rows // CHUNK
    tall = rows + 2 * EDGE
    f32 = jnp.float32
    hbm = pl.BlockSpec(memory_space=pltpu.HBM)
    vmem = pl.BlockSpec(memory_space=pltpu.VMEM)
    dma = pltpu.SemaphoreType.DMA
    result = jax.ShapeDtypeStruct((2, depth, width, LANES), f32)
    return pl.pallas_call(
        kernel,
        out_shape=(result, result),
        in_specs=[hbm] * 5,
        out_specs=(vmem, vmem),
        scratch_shapes=[
            pltpu.VMEM((4, depth + 2, tall, LANES), f32),
            pltpu.VMEM((4, depth + 2, tall, LANES), f32),
            pltpu.VMEM((4, depth, rows, LANES), f32),
            pltpu.VMEM((2, depth, rows, LANES), f32),
            pltpu.VMEM((depth, rows, LANES), f32),
            pltpu.VMEM((depth, rows, LANES), f32),
            pltpu.VMEM((depth + 2, tall, LANES), jnp.int32),
            pltpu.VMEM((depth + 2, tall, LANES), f32),
            pltpu.VMEM((7, depth, rows, LANES), f32),
            pltpu.VMEM((depth, rows, LANES), f32),
            pltpu.VMEM((2, depth, LANES), f32),
            pltpu.VMEM((2, depth, LANES), f32),
            pltpu.VMEM((4, depth, LANES), f32),
            pltpu.VMEM((4, depth, LANES), f32),
            dma((7,)),
            dma((2,)),
            dma((2,)),
            dma((2,)),
            dma((2,)),
            dma((2, chunks)),
            dma((2, chunks)),
            dma((2, 2, chunks)),
            dma((2, 2, chunks)),
            dma((2,)),
            dma((2,)),
            dma((2, chunks)),
            dma((2, chunks)),
            dma((2, chunks)),
            dma((2, chunks)),
        ],
        compiler_params=pltpu.CompilerParams(
            collective_id=0, has_side_effects=True, vmem_limit_bytes=24 * 1024 * 1024
        ),
    )(*[pltpu.with_memory_space_constraint(x, pltpu.HBM) for x in arguments])


def solution(mesh):
    return jax.shard_map(
        on_device,
        mesh=mesh,
        in_specs=(
            P("space", None, None),
            P("space", None, None),
            P("space", None, None),
            P("node", "space", None, None),
            P("node", "space", None, None),
        ),
        out_specs=(P("node", "space", None, None), P("node", "space", None, None)),
        check_vma=False,
    )
```

```python
import jax
import jax.numpy as jnp
from jax import lax
from jax.experimental import pallas as pl
from jax.experimental.pallas import tpu as pltpu
from jax.sharding import PartitionSpec as P

MESH = pl.DeviceIdType.MESH
LANES = 128
CHUNK = 32
STEP = 16
EDGE = 8
LAG = 1

radau_points = (0.08858795951270396, 0.4094668644407347, 0.7876594617608471, 1.0)
time_step = 0.16
onset_level = 0.15
ionic_gain = 8.0
recovery_base = 0.002
recovery_slope = 0.2
recovery_offset = 0.3
conductances = (1.0, 0.35, 0.05)
excitability = (1.0, 0.6, 0.0)


def weight_table():
    table = []
    for target in range(4):
        entries = []
        for column in range(4):
            coeffs = [1.0]
            for other in range(4):
                if other != column:
                    factor = 1.0 / (radau_points[column] - radau_points[other])
                    raised = [0.0] + coeffs
                    lowered = coeffs + [0.0]
                    coeffs = [
                        factor * (raised[place] - radau_points[other] * lowered[place])
                        for place in range(len(raised))
                    ]
            integral = 0.0
            for place in range(len(coeffs)):
                integral = integral + coeffs[place] * radau_points[target] ** (place + 1) / (
                    place + 1
                )
            entries.append(time_step * integral)
        table.append(entries)
    return table


def label_values(labels, values, outside):
    return jnp.where(
        labels == 0,
        jnp.float32(values[0]),
        jnp.where(
            labels == 1,
            jnp.float32(values[1]),
            jnp.where(labels == 2, jnp.float32(values[2]), jnp.float32(outside)),
        ),
    )


def kernel(
    us_hbm,
    vs_hbm,
    lab_hbm,
    ug_hbm,
    vg_hbm,
    out_u,
    out_v,
    u0,
    u1,
    v,
    res,
    us,
    vs,
    lab,
    cond,
    face,
    exc,
    b0s,
    b0r,
    b1s,
    b1r,
    load_sem,
    lab_send,
    lab_recv,
    side_send,
    halo_recv,
    mid_recv,
    row_send,
    row_recv,
    in_send,
    in_recv,
    back_send,
    back_recv,
):
    depth, rows = lab_hbm.shape[0], lab_hbm.shape[1] // 2
    chunks = rows // CHUNK
    node, here = lax.axis_index("node"), lax.axis_index("space")
    count = lax.axis_size("space")
    fold = count // 2
    half = lax.rem(node + here // fold, 2)
    own, other = half * rows, (1 - half) * rows
    has = (here > 0, here < count - 1)
    flips = ((here == fold).astype(jnp.int32), (here == fold - 1).astype(jnp.int32))
    sides = (
        (lax.rem(node + flips[0], 2), here - 1),
        (lax.rem(node + flips[1], 2), here + 1),
    )
    partner = (1 - node, here)
    ours = (1, depth)
    theirs = (depth + 1, 0)

    def mine(k):
        return k * half + (chunks - 1 - k) * (1 - half)

    def its(k):
        return k * (1 - half) + (chunks - 1 - k) * half

    def rows_of(c, base):
        return pl.ds(pl.multiple_of(base + CHUNK * c, 8), CHUNK)

    def step_of(row):
        return pl.ds(pl.multiple_of(row, 8), STEP)

    def remote(src, dst, send, recv, device):
        return pltpu.make_async_remote_copy(
            src_ref=src,
            dst_ref=dst,
            send_sem=send,
            recv_sem=recv,
            device_id=device,
            device_id_type=MESH,
        )

    own_rows = pl.ds(pl.multiple_of(own, 8), rows)
    inner = pl.ds(EDGE, rows)
    slab = pl.ds(1, depth)
    edge_source = pl.ds(pl.multiple_of(rows - EDGE * half, 8), EDGE)
    edge_place = pl.ds(pl.multiple_of((EDGE + rows) * (1 - half), 8), EDGE)
    void_place = pl.ds(pl.multiple_of((EDGE + rows) * half, 8), EDGE)

    def lab_copy(side):
        return remote(
            lab_hbm.at[pl.ds(ours[side] - 1, 1), own_rows],
            lab.at[pl.ds(theirs[side], 1), inner],
            lab_send.at[side],
            lab_recv.at[1 - side],
            sides[side],
        )

    def own_copy(side):
        return remote(
            ug_hbm.at[:, pl.ds(ours[side] - 1, 1), own_rows],
            u0.at[pl.ds(2 * flips[side], 2), pl.ds(theirs[side], 1), inner],
            side_send.at[side],
            halo_recv.at[1 - side],
            sides[side],
        )

    def fwd_copy(side, k):
        at = rows_of(mine(k), EDGE)
        return remote(
            u0.at[pl.ds(2, 2), pl.ds(ours[side], 1), at],
            u0.at[pl.ds(2 - 2 * flips[side], 2), pl.ds(theirs[side], 1), at],
            side_send.at[side],
            halo_recv.at[1 - side],
            sides[side],
        )

    def mid_copy(side, pair, k):
        at = rows_of(mine(k), EDGE)
        to = 2 * (pair + flips[side] - 2 * pair * flips[side])
        return remote(
            u1.at[pl.ds(2 * pair, 2), pl.ds(ours[side], 1), at],
            u1.at[pl.ds(to, 2), pl.ds(theirs[side], 1), at],
            side_send.at[side],
            mid_recv.at[1 - side, k],
            sides[side],
        )

    def in_copy(field, k, c, base):
        return remote(
            (ug_hbm, vg_hbm)[field].at[:, :, rows_of(c, base)],
            (
                u0.at[pl.ds(2, 2), slab, rows_of(c, EDGE)],
                v.at[pl.ds(2, 2), :, rows_of(c, 0)],
            )[field],
            in_send.at[0],
            in_recv.at[field, k],
            partner,
        )

    def sent(field, k):
        return in_copy(field, k, its(k), other)

    def arriving(field, k):
        return in_copy(field, k, mine(k), own)

    def back_copies(c, base):
        return (
            remote(
                res.at[:, :, rows_of(c, 0)],
                out_u.at[:, :, rows_of(c, base)],
                back_send.at[0],
                back_recv.at[0],
                partner,
            ),
            remote(
                v.at[pl.ds(2, 2), :, rows_of(c, 0)],
                out_v.at[:, :, rows_of(c, base)],
                back_send.at[0],
                back_recv.at[0],
                partner,
            ),
        )

    row_copies = (
        remote(b0s, b0r, row_send.at[0], row_recv.at[0], partner),
        remote(b1s, b1r, row_send.at[1], row_recv.at[1], partner),
    )

    loads = [
        pltpu.make_async_copy(src, dst, load_sem.at[i])
        for i, src, dst in (
            (0, ug_hbm.at[:, :, own_rows], u0.at[pl.ds(0, 2), slab, inner]),
            (0, ug_hbm.at[:, :, edge_source], u0.at[pl.ds(0, 2), slab, edge_place]),
            (1, lab_hbm.at[:, own_rows], lab.at[slab, inner]),
            (1, lab_hbm.at[:, edge_source], lab.at[slab, edge_place]),
            (2, vg_hbm.at[:, :, own_rows], v.at[pl.ds(0, 2)]),
            (2, us_hbm.at[:, own_rows], us),
            (2, vs_hbm.at[:, own_rows], vs),
        )
    ]
    grown = pl.ds(pl.multiple_of(EDGE * (1 - half), 8), EDGE + rows)

    def await_bytes(ref, sem):
        pltpu.make_async_copy(ref, ref, sem).wait()

    barrier = pltpu.get_barrier_semaphore()
    pl.semaphore_signal(barrier, inc=1, device_id=partner, device_id_type=MESH)
    for side in (0, 1):

        @pl.when(has[side])
        def _():
            pl.semaphore_signal(barrier, inc=1, device_id=sides[side], device_id_type=MESH)

    for copy in loads[:2]:
        copy.start()
    pl.semaphore_wait(barrier, 1 + has[0].astype(jnp.int32) + has[1].astype(jnp.int32))

    for k in range(2):
        sent(0, k).start()
    for copy in loads[2:]:
        copy.start()
    for side in (0, 1):

        @pl.when(has[side])
        def _():
            lab_copy(side).start()
            own_copy(side).start()

    def take_row(source, target, nodes):
        @pl.when(half == 0)
        def _():
            for j in range(nodes):
                for p in range(depth):
                    target[j, p : p + 1] = source[j, p + 1, EDGE + rows - 1 : EDGE + rows]

        @pl.when(half == 1)
        def _():
            for j in range(nodes):
                for p in range(depth):
                    target[j, p : p + 1] = source[j, p + 1, EDGE : EDGE + 1]

    def put_row(source, target, nodes, first):
        @pl.when(half == 0)
        def _():
            for j in range(nodes):
                for p in range(depth):
                    target[first(j), p + 1, EDGE + rows : EDGE + rows + 1] = source[j, p : p + 1]

        @pl.when(half == 1)
        def _():
            for j in range(nodes):
                for p in range(depth):
                    target[first(j), p + 1, EDGE - 1 : EDGE] = source[j, p : p + 1]

    await_bytes(u0.at[pl.ds(0, 2), slab, grown], load_sem.at[0])
    take_row(u0, b0s, 2)
    row_copies[0].start()

    @pl.loop(2, chunks)
    def _(k):
        sent(0, k).start()

    @pl.loop(0, chunks)
    def _(k):
        sent(1, k).start()

    for place in range(4):
        for p in range(depth):
            u0[place, p + 1, void_place] = jnp.zeros((EDGE, LANES), jnp.float32)
            u1[place, p + 1, void_place] = jnp.zeros((EDGE, LANES), jnp.float32)
    for p in range(depth):
        lab[p + 1, void_place] = jnp.full((EDGE, LANES), 3, jnp.int32)
    for side in (0, 1):

        @pl.when(jnp.logical_not(has[side]))
        def _():
            plane = (0, depth + 1)[side]

            @pl.loop(0, chunks)
            def _(c):
                at = rows_of(c, EDGE)
                lab[plane, at] = jnp.full((CHUNK, LANES), 3, jnp.int32)
                for place in range(4):
                    u0[place, plane, at] = jnp.zeros((CHUNK, LANES), jnp.float32)
                    u1[place, plane, at] = jnp.zeros((CHUNK, LANES), jnp.float32)

    await_bytes(lab.at[slab, grown], load_sem.at[1])
    for side in (0, 1):

        @pl.when(has[side])
        def _():
            lab_copy(1 - side).wait_recv()

    @pl.loop(0, depth + 2)
    def _(p):
        for c in range(chunks):
            at = pl.ds(EDGE + CHUNK * c, CHUNK)
            cond[p, at] = label_values(lab[p, at], conductances, 0.0)

    for p in range(depth):
        for at in (pl.ds(0, EDGE), pl.ds(EDGE + rows, EDGE)):
            cond[p + 1, at] = label_values(lab[p + 1, at], conductances, 0.0)

    lane = lax.broadcasted_iota(jnp.int32, (STEP, LANES), 1)

    @pl.loop(0, depth)
    def _(p):
        @pl.loop(0, rows // STEP)
        def _(i):
            at, to = step_of(EDGE + STEP * i), step_of(STEP * i)
            row = EDGE + STEP * i
            center = cond[p + 1, at]
            beside = (
                cond[p + 2, at],
                cond[p, at],
                cond[p + 1, pl.ds(row + 1, STEP)],
                cond[p + 1, pl.ds(row - 1, STEP)],
                jnp.where(lane == LANES - 1, 0.0, pltpu.roll(center, LANES - 1, 1)),
                jnp.where(lane == 0, 0.0, pltpu.roll(center, 1, 1)),
            )
            total = jnp.zeros_like(center)
            for f in range(6):
                value = 2.0 * center * beside[f] / (center + beside[f])
                face[f, p, to] = value
                total = total + value
            face[6, p, to] = total
            exc[p, to] = label_values(lab[p + 1, at], excitability, 0.0)

    await_bytes(v, load_sem.at[2])
    row_copies[0].wait_recv()
    put_row(b0r, u0, 2, lambda j: 2 + j)

    @pl.loop(0, chunks)
    def _(k):
        arriving(0, k).wait_recv()
        for side in (0, 1):

            @pl.when(has[side])
            def _():
                fwd_copy(side, k).start()

    for side in (0, 1):

        @pl.when(has[side])
        def _():
            await_bytes(u0.at[:, pl.ds(theirs[1 - side], 1), inner], halo_recv.at[side])

    table = weight_table()
    weights = [
        [
            jnp.where(
                node == 0,
                jnp.float32(table[m][j]),
                jnp.float32(table[(m + 2) % 4][(j + 2) % 4]),
            )
            for j in range(4)
        ]
        for m in range(4)
    ]

    def sweep(source, c, write):
        @pl.loop(0, depth * (CHUNK // STEP))
        def _(i):
            p, first = i % depth, CHUNK * c + STEP * (i // depth)
            at, to = step_of(EDGE + first), step_of(first)
            row = EDGE + first
            faces = [face[f, p, to] for f in range(7)]
            excite = exc[p, to]
            sum_u = [us[p, to]] * 4
            sum_v = [vs[p, to]] * 4
            for j in range(4):
                mid = source[j, p + 1, at]
                v_mid = v[j, p, to]
                spread = (
                    faces[0] * source[j, p + 2, at]
                    + faces[1] * source[j, p, at]
                    + faces[2] * source[j, p + 1, pl.ds(row + 1, STEP)]
                    + faces[3] * source[j, p + 1, pl.ds(row - 1, STEP)]
                    + faces[4] * pltpu.roll(mid, LANES - 1, 1)
                    + faces[5] * pltpu.roll(mid, 1, 1)
                )
                scaled = ionic_gain * mid
                growth = (scaled - ionic_gain * onset_level) * (1.0 - mid) - v_mid
                rate_u = spread + mid * (excite * growth - faces[6])
                recovery = recovery_base + recovery_slope * v_mid / jnp.maximum(
                    mid + recovery_offset, recovery_offset
                )
                rate_v = recovery * (-v_mid - scaled * (mid - (onset_level + 1.0)))
                for m in range(4):
                    sum_u[m] = sum_u[m] + weights[m][j] * rate_u
                    sum_v[m] = sum_v[m] + weights[m][j] * rate_v
            write(p, first, sum_u, sum_v)

    def first_sweep(k):
        c = mine(k)

        def write(p, first, new_u, new_v):
            at, to = step_of(EDGE + first), step_of(first)
            for m in range(4):
                u1[m, p + 1, at] = new_u[m]
                v[m, p, to] = new_v[m]

        sweep(u0, c, write)

    def second_sweep(k):
        c = mine(k)
        for side in (0, 1):

            @pl.when(has[side])
            def _():
                at = rows_of(c, EDGE)
                await_bytes(u1.at[:, pl.ds(theirs[1 - side], 1), at], mid_recv.at[side, k])

        def write(p, first, new_u, new_v):
            to, full = step_of(first), step_of(own + first)
            for m in range(2):
                out_u[m, p, full] = new_u[m]
                out_v[m, p, full] = new_v[m]
                res[m, p, to] = new_u[2 + m]
                v[2 + m, p, to] = new_v[2 + m]

        sweep(u1, c, write)
        for copy in back_copies(c, own):
            copy.start()

    @pl.loop(0, chunks)
    def _(k):
        arriving(1, k).wait_recv()
        first_sweep(k)
        for side in (0, 1):

            @pl.when(has[side])
            def _():
                for pair in (0, 1):
                    mid_copy(side, pair, k).start()

        @pl.when(k == 0)
        def _():
            take_row(u1, b1s, 4)
            row_copies[1].start()

        @pl.when(k > LAG)
        def _():
            second_sweep(k - LAG)

    @pl.loop(chunks - LAG, chunks)
    def _(k):
        second_sweep(k)

    row_copies[1].wait_recv()
    put_row(b1r, u1, 4, lambda j: (j + 2) % 4)
    second_sweep(0)

    for side in (0, 1):

        @pl.when(has[side])
        def _():
            lab_copy(side).wait_send()
            await_bytes(u1.at[:, pl.ds(0, 2), inner], side_send.at[side])

    for copy in row_copies:
        copy.wait_send()
    await_bytes(v, in_send.at[0])
    await_bytes(v, back_send.at[0])
    await_bytes(v, back_recv.at[0])


def on_device(*arguments):
    labels = arguments[2]
    depth, width = labels.shape[0], labels.shape[1]
    rows = width // 2
    chunks = rows // CHUNK
    tall = rows + 2 * EDGE
    f32 = jnp.float32
    hbm = pl.BlockSpec(memory_space=pltpu.HBM)
    vmem = pl.BlockSpec(memory_space=pltpu.VMEM)
    dma = pltpu.SemaphoreType.DMA
    result = jax.ShapeDtypeStruct((2, depth, width, LANES), f32)
    return pl.pallas_call(
        kernel,
        out_shape=(result, result),
        in_specs=[hbm] * 5,
        out_specs=(vmem, vmem),
        scratch_shapes=[
            pltpu.VMEM((4, depth + 2, tall, LANES), f32),
            pltpu.VMEM((4, depth + 2, tall, LANES), f32),
            pltpu.VMEM((4, depth, rows, LANES), f32),
            pltpu.VMEM((2, depth, rows, LANES), f32),
            pltpu.VMEM((depth, rows, LANES), f32),
            pltpu.VMEM((depth, rows, LANES), f32),
            pltpu.VMEM((depth + 2, tall, LANES), jnp.int32),
            pltpu.VMEM((depth + 2, tall, LANES), f32),
            pltpu.VMEM((7, depth, rows, LANES), f32),
            pltpu.VMEM((depth, rows, LANES), f32),
            pltpu.VMEM((2, depth, LANES), f32),
            pltpu.VMEM((2, depth, LANES), f32),
            pltpu.VMEM((4, depth, LANES), f32),
            pltpu.VMEM((4, depth, LANES), f32),
            dma((3,)),
            dma((2,)),
            dma((2,)),
            dma((2,)),
            dma((2,)),
            dma((2, chunks)),
            dma((2,)),
            dma((2,)),
            dma((1,)),
            dma((2, chunks)),
            dma((1,)),
            dma((1,)),
        ],
        compiler_params=pltpu.CompilerParams(
            collective_id=0, has_side_effects=True, vmem_limit_bytes=24 * 1024 * 1024
        ),
    )(*[pltpu.with_memory_space_constraint(x, pltpu.HBM) for x in arguments])


def solution(mesh):
    return jax.shard_map(
        on_device,
        mesh=mesh,
        in_specs=(
            P("space", None, None),
            P("space", None, None),
            P("space", None, None),
            P("node", "space", None, None),
            P("node", "space", None, None),
        ),
        out_specs=(P("node", "space", None, None), P("node", "space", None, None)),
        check_vma=False,
    )
```

```python
import jax
import jax.numpy as jnp
from jax import lax
from jax.experimental import pallas as pl
from jax.experimental.pallas import tpu as pltpu
from jax.sharding import PartitionSpec as P

MESH = pl.DeviceIdType.MESH
LANES = 128
CHUNK = 32
STEP = 16
EDGE = 8
LAG = 1

radau_points = (0.08858795951270396, 0.4094668644407347, 0.7876594617608471, 1.0)
time_step = 0.16
onset_level = 0.15
ionic_gain = 8.0
recovery_base = 0.002
recovery_slope = 0.2
recovery_offset = 0.3
conductances = (1.0, 0.35, 0.05)
excitability = (1.0, 0.6, 0.0)


def weight_table():
    table = []
    for target in range(4):
        entries = []
        for column in range(4):
            coeffs = [1.0]
            for other in range(4):
                if other != column:
                    factor = 1.0 / (radau_points[column] - radau_points[other])
                    raised = [0.0] + coeffs
                    lowered = coeffs + [0.0]
                    coeffs = [
                        factor * (raised[place] - radau_points[other] * lowered[place])
                        for place in range(len(raised))
                    ]
            integral = 0.0
            for place in range(len(coeffs)):
                integral = integral + coeffs[place] * radau_points[target] ** (place + 1) / (
                    place + 1
                )
            entries.append(time_step * integral)
        table.append(entries)
    return table


def label_values(labels, values, outside):
    return jnp.where(
        labels == 0,
        jnp.float32(values[0]),
        jnp.where(
            labels == 1,
            jnp.float32(values[1]),
            jnp.where(labels == 2, jnp.float32(values[2]), jnp.float32(outside)),
        ),
    )


def kernel(
    us_hbm,
    vs_hbm,
    lab_hbm,
    ug_hbm,
    vg_hbm,
    out_u,
    out_v,
    u0,
    u1,
    v,
    res,
    us,
    vs,
    lab,
    cond,
    face,
    exc,
    b0s,
    b0r,
    b1s,
    b1r,
    load_sem,
    lab_send,
    lab_recv,
    side_send,
    halo_recv,
    mid_recv,
    row_send,
    row_recv,
    in_send,
    in_recv,
    back_send,
    back_recv,
    hello,
    met,
):
    depth, rows = lab_hbm.shape[0], lab_hbm.shape[1] // 2
    chunks = rows // CHUNK
    node, here = lax.axis_index("node"), lax.axis_index("space")
    count = lax.axis_size("space")
    fold = count // 2
    half = lax.rem(node + here // fold, 2)
    own, other = half * rows, (1 - half) * rows
    has = (here > 0, here < count - 1)
    flips = ((here == fold).astype(jnp.int32), (here == fold - 1).astype(jnp.int32))
    sides = (
        (lax.rem(node + flips[0], 2), here - 1),
        (lax.rem(node + flips[1], 2), here + 1),
    )
    partner = (1 - node, here)
    ours = (1, depth)
    theirs = (depth + 1, 0)

    def mine(k):
        return k * half + (chunks - 1 - k) * (1 - half)

    def its(k):
        return k * (1 - half) + (chunks - 1 - k) * half

    def rows_of(c, base):
        return pl.ds(pl.multiple_of(base + CHUNK * c, 8), CHUNK)

    def step_of(row):
        return pl.ds(pl.multiple_of(row, 8), STEP)

    def remote(src, dst, send, recv, device):
        return pltpu.make_async_remote_copy(
            src_ref=src,
            dst_ref=dst,
            send_sem=send,
            recv_sem=recv,
            device_id=device,
            device_id_type=MESH,
        )

    own_rows = pl.ds(pl.multiple_of(own, 8), rows)
    inner = pl.ds(EDGE, rows)
    slab = pl.ds(1, depth)
    edge_source = pl.ds(pl.multiple_of(rows - EDGE * half, 8), EDGE)
    edge_place = pl.ds(pl.multiple_of((EDGE + rows) * (1 - half), 8), EDGE)
    void_place = pl.ds(pl.multiple_of((EDGE + rows) * half, 8), EDGE)

    def lab_copy(side):
        return remote(
            lab_hbm.at[pl.ds(ours[side] - 1, 1), own_rows],
            lab.at[pl.ds(theirs[side], 1), inner],
            lab_send.at[side],
            lab_recv.at[1 - side],
            sides[side],
        )

    def own_copy(side):
        return remote(
            ug_hbm.at[:, pl.ds(ours[side] - 1, 1), own_rows],
            u0.at[pl.ds(2 * flips[side], 2), pl.ds(theirs[side], 1), inner],
            side_send.at[side],
            halo_recv.at[1 - side],
            sides[side],
        )

    def fwd_copy(side, k):
        at = rows_of(mine(k), EDGE)
        return remote(
            u0.at[pl.ds(2, 2), pl.ds(ours[side], 1), at],
            u0.at[pl.ds(2 - 2 * flips[side], 2), pl.ds(theirs[side], 1), at],
            side_send.at[side],
            halo_recv.at[1 - side],
            sides[side],
        )

    def mid_copy(side, pair, k):
        at = rows_of(mine(k), EDGE)
        to = 2 * (pair + flips[side] - 2 * pair * flips[side])
        return remote(
            u1.at[pl.ds(2 * pair, 2), pl.ds(ours[side], 1), at],
            u1.at[pl.ds(to, 2), pl.ds(theirs[side], 1), at],
            side_send.at[side],
            mid_recv.at[1 - side, k],
            sides[side],
        )

    def in_copy(field, k, c, base):
        return remote(
            (ug_hbm, vg_hbm)[field].at[:, :, rows_of(c, base)],
            (
                u0.at[pl.ds(2, 2), slab, rows_of(c, EDGE)],
                v.at[pl.ds(2, 2), :, rows_of(c, 0)],
            )[field],
            in_send.at[0],
            in_recv.at[field, k],
            partner,
        )

    def sent(field, k):
        return in_copy(field, k, its(k), other)

    def arriving(field, k):
        return in_copy(field, k, mine(k), own)

    def back_copies(c, base):
        return (
            remote(
                res.at[:, :, rows_of(c, 0)],
                out_u.at[:, :, rows_of(c, base)],
                back_send.at[0],
                back_recv.at[0],
                partner,
            ),
            remote(
                v.at[pl.ds(2, 2), :, rows_of(c, 0)],
                out_v.at[:, :, rows_of(c, base)],
                back_send.at[0],
                back_recv.at[0],
                partner,
            ),
        )

    row_copies = (
        remote(b0s, b0r, row_send.at[0], row_recv.at[0], partner),
        remote(b1s, b1r, row_send.at[1], row_recv.at[1], partner),
    )

    loads = [
        pltpu.make_async_copy(src, dst, load_sem.at[i])
        for i, src, dst in (
            (0, ug_hbm.at[:, :, own_rows], u0.at[pl.ds(0, 2), slab, inner]),
            (0, ug_hbm.at[:, :, edge_source], u0.at[pl.ds(0, 2), slab, edge_place]),
            (1, lab_hbm.at[:, own_rows], lab.at[slab, inner]),
            (1, lab_hbm.at[:, edge_source], lab.at[slab, edge_place]),
            (2, vg_hbm.at[:, :, own_rows], v.at[pl.ds(0, 2)]),
            (2, us_hbm.at[:, own_rows], us),
            (2, vs_hbm.at[:, own_rows], vs),
        )
    ]
    grown = pl.ds(pl.multiple_of(EDGE * (1 - half), 8), EDGE + rows)

    def await_bytes(ref, sem):
        pltpu.make_async_copy(ref, ref, sem).wait()

    odd, first = here % 2 == 1, node == 1
    host = jnp.logical_and(odd, jnp.logical_not(first))
    guest = jnp.logical_and(odd, first)
    barrier = pltpu.get_barrier_semaphore()

    def signal(sem, device):
        pl.semaphore_signal(sem, inc=1, device_id=device, device_id_type=MESH)

    for copy in loads[:2]:
        copy.start()

    @pl.when(jnp.logical_not(guest))
    def _():
        signal(barrier, partner)

    @pl.when(jnp.logical_not(host))
    def _():
        pl.semaphore_wait(barrier, 1)

    @pl.when(guest)
    def _():
        signal(hello, partner)

    @pl.when(host)
    def _():
        pl.semaphore_wait(hello, 1)

    for k in range(2):
        sent(0, k).start()
    for copy in loads[2:]:
        copy.start()
    for side in (0, 1):

        @pl.when(jnp.logical_and(has[side], jnp.logical_not(jnp.logical_or(odd, sides[side][0] == 1))))
        def _():
            signal(barrier, sides[side])

    def take_row(source, target, nodes):
        @pl.when(half == 0)
        def _():
            for j in range(nodes):
                for p in range(depth):
                    target[j, p : p + 1] = source[j, p + 1, EDGE + rows - 1 : EDGE + rows]

        @pl.when(half == 1)
        def _():
            for j in range(nodes):
                for p in range(depth):
                    target[j, p : p + 1] = source[j, p + 1, EDGE : EDGE + 1]

    def put_row(source, target, nodes, first):
        @pl.when(half == 0)
        def _():
            for j in range(nodes):
                for p in range(depth):
                    target[first(j), p + 1, EDGE + rows : EDGE + rows + 1] = source[j, p : p + 1]

        @pl.when(half == 1)
        def _():
            for j in range(nodes):
                for p in range(depth):
                    target[first(j), p + 1, EDGE - 1 : EDGE] = source[j, p : p + 1]

    await_bytes(u0.at[pl.ds(0, 2), slab, grown], load_sem.at[0])
    take_row(u0, b0s, 2)
    row_copies[0].start()

    @pl.loop(2, chunks)
    def _(k):
        sent(0, k).start()

    @pl.loop(0, chunks)
    def _(k):
        sent(1, k).start()

    beside_count = has[0].astype(jnp.int32) + has[1].astype(jnp.int32)

    @pl.when(host)
    def _():
        pl.semaphore_wait(barrier, beside_count)
        signal(met, partner)

    @pl.when(guest)
    def _():
        pl.semaphore_wait(met, 1)

    for side in (0, 1):

        @pl.when(jnp.logical_and(odd, has[side]))
        def _():
            signal(met, sides[side])

    @pl.when(jnp.logical_not(odd))
    def _():
        pl.semaphore_wait(met, beside_count)

    for side in (0, 1):

        @pl.when(has[side])
        def _():
            lab_copy(side).start()
            own_copy(side).start()

    for place in range(4):
        for p in range(depth):
            u0[place, p + 1, void_place] = jnp.zeros((EDGE, LANES), jnp.float32)
            u1[place, p + 1, void_place] = jnp.zeros((EDGE, LANES), jnp.float32)
    for p in range(depth):
        lab[p + 1, void_place] = jnp.full((EDGE, LANES), 3, jnp.int32)
    for side in (0, 1):

        @pl.when(jnp.logical_not(has[side]))
        def _():
            plane = (0, depth + 1)[side]

            @pl.loop(0, chunks)
            def _(c):
                at = rows_of(c, EDGE)
                lab[plane, at] = jnp.full((CHUNK, LANES), 3, jnp.int32)
                for place in range(4):
                    u0[place, plane, at] = jnp.zeros((CHUNK, LANES), jnp.float32)
                    u1[place, plane, at] = jnp.zeros((CHUNK, LANES), jnp.float32)

    await_bytes(lab.at[slab, grown], load_sem.at[1])
    for side in (0, 1):

        @pl.when(has[side])
        def _():
            lab_copy(1 - side).wait_recv()

    @pl.loop(0, depth + 2)
    def _(p):
        for c in range(chunks):
            at = pl.ds(EDGE + CHUNK * c, CHUNK)
            cond[p, at] = label_values(lab[p, at], conductances, 0.0)

    for p in range(depth):
        for at in (pl.ds(0, EDGE), pl.ds(EDGE + rows, EDGE)):
            cond[p + 1, at] = label_values(lab[p + 1, at], conductances, 0.0)

    lane = lax.broadcasted_iota(jnp.int32, (STEP, LANES), 1)

    @pl.loop(0, depth)
    def _(p):
        @pl.loop(0, rows // STEP)
        def _(i):
            at, to = step_of(EDGE + STEP * i), step_of(STEP * i)
            row = EDGE + STEP * i
            center = cond[p + 1, at]
            beside = (
                cond[p + 2, at],
                cond[p, at],
                cond[p + 1, pl.ds(row + 1, STEP)],
                cond[p + 1, pl.ds(row - 1, STEP)],
                jnp.where(lane == LANES - 1, 0.0, pltpu.roll(center, LANES - 1, 1)),
                jnp.where(lane == 0, 0.0, pltpu.roll(center, 1, 1)),
            )
            total = jnp.zeros_like(center)
            for f in range(6):
                value = 2.0 * center * beside[f] / (center + beside[f])
                face[f, p, to] = value
                total = total + value
            face[6, p, to] = total
            exc[p, to] = label_values(lab[p + 1, at], excitability, 0.0)

    await_bytes(v, load_sem.at[2])
    row_copies[0].wait_recv()
    put_row(b0r, u0, 2, lambda j: 2 + j)

    @pl.loop(0, chunks)
    def _(k):
        arriving(0, k).wait_recv()
        for side in (0, 1):

            @pl.when(has[side])
            def _():
                fwd_copy(side, k).start()

    for side in (0, 1):

        @pl.when(has[side])
        def _():
            await_bytes(u0.at[:, pl.ds(theirs[1 - side], 1), inner], halo_recv.at[side])

    table = weight_table()
    weights = [
        [
            jnp.where(
                node == 0,
                jnp.float32(table[m][j]),
                jnp.float32(table[(m + 2) % 4][(j + 2) % 4]),
            )
            for j in range(4)
        ]
        for m in range(4)
    ]

    def sweep(source, c, write):
        @pl.loop(0, depth * (CHUNK // STEP))
        def _(i):
            p, first = i % depth, CHUNK * c + STEP * (i // depth)
            at, to = step_of(EDGE + first), step_of(first)
            row = EDGE + first
            faces = [face[f, p, to] for f in range(7)]
            excite = exc[p, to]
            sum_u = [us[p, to]] * 4
            sum_v = [vs[p, to]] * 4
            for j in range(4):
                mid = source[j, p + 1, at]
                v_mid = v[j, p, to]
                spread = (
                    faces[0] * source[j, p + 2, at]
                    + faces[1] * source[j, p, at]
                    + faces[2] * source[j, p + 1, pl.ds(row + 1, STEP)]
                    + faces[3] * source[j, p + 1, pl.ds(row - 1, STEP)]
                    + faces[4] * pltpu.roll(mid, LANES - 1, 1)
                    + faces[5] * pltpu.roll(mid, 1, 1)
                )
                scaled = ionic_gain * mid
                growth = (scaled - ionic_gain * onset_level) * (1.0 - mid) - v_mid
                rate_u = spread + mid * (excite * growth - faces[6])
                recovery = recovery_base + recovery_slope * v_mid / jnp.maximum(
                    mid + recovery_offset, recovery_offset
                )
                rate_v = recovery * (-v_mid - scaled * (mid - (onset_level + 1.0)))
                for m in range(4):
                    sum_u[m] = sum_u[m] + weights[m][j] * rate_u
                    sum_v[m] = sum_v[m] + weights[m][j] * rate_v
            write(p, first, sum_u, sum_v)

    def first_sweep(k):
        c = mine(k)

        def write(p, first, new_u, new_v):
            at, to = step_of(EDGE + first), step_of(first)
            for m in range(4):
                u1[m, p + 1, at] = new_u[m]
                v[m, p, to] = new_v[m]

        sweep(u0, c, write)

    def second_sweep(k):
        c = mine(k)
        for side in (0, 1):

            @pl.when(has[side])
            def _():
                at = rows_of(c, EDGE)
                await_bytes(u1.at[:, pl.ds(theirs[1 - side], 1), at], mid_recv.at[side, k])

        def write(p, first, new_u, new_v):
            to, full = step_of(first), step_of(own + first)
            for m in range(2):
                out_u[m, p, full] = new_u[m]
                out_v[m, p, full] = new_v[m]
                res[m, p, to] = new_u[2 + m]
                v[2 + m, p, to] = new_v[2 + m]

        sweep(u1, c, write)
        for copy in back_copies(c, own):
            copy.start()

    @pl.loop(0, chunks)
    def _(k):
        arriving(1, k).wait_recv()
        first_sweep(k)
        for side in (0, 1):

            @pl.when(has[side])
            def _():
                for pair in (0, 1):
                    mid_copy(side, pair, k).start()

        @pl.when(k == 0)
        def _():
            take_row(u1, b1s, 4)
            row_copies[1].start()

        @pl.when(k > LAG)
        def _():
            second_sweep(k - LAG)

    @pl.loop(chunks - LAG, chunks)
    def _(k):
        second_sweep(k)

    row_copies[1].wait_recv()
    put_row(b1r, u1, 4, lambda j: (j + 2) % 4)
    second_sweep(0)

    for side in (0, 1):

        @pl.when(has[side])
        def _():
            lab_copy(side).wait_send()
            await_bytes(u1.at[:, pl.ds(0, 2), inner], side_send.at[side])

    for copy in row_copies:
        copy.wait_send()
    await_bytes(v, in_send.at[0])
    await_bytes(v, back_send.at[0])
    await_bytes(v, back_recv.at[0])


def store(u_vmem, v_vmem, u_hbm, v_hbm, sem):
    copies = [
        pltpu.make_async_copy(src.at[m, p], dst.at[m, p], sem.at[2 * i + m])
        for i, (src, dst) in enumerate(((u_vmem, u_hbm), (v_vmem, v_hbm)))
        for m in range(2)
        for p in range(u_vmem.shape[1])
    ]
    for copy in copies:
        copy.start()
    for copy in copies:
        copy.wait()


def on_device(*arguments):
    labels = arguments[2]
    depth, width = labels.shape[0], labels.shape[1]
    rows = width // 2
    chunks = rows // CHUNK
    tall = rows + 2 * EDGE
    f32 = jnp.float32
    hbm = pl.BlockSpec(memory_space=pltpu.HBM)
    vmem = pl.BlockSpec(memory_space=pltpu.VMEM)
    dma = pltpu.SemaphoreType.DMA
    result = jax.ShapeDtypeStruct((2, depth, width, LANES), f32)
    results = pl.pallas_call(
        kernel,
        out_shape=(result, result),
        in_specs=[hbm] * 5,
        out_specs=(vmem, vmem),
        scratch_shapes=[
            pltpu.VMEM((4, depth + 2, tall, LANES), f32),
            pltpu.VMEM((4, depth + 2, tall, LANES), f32),
            pltpu.VMEM((4, depth, rows, LANES), f32),
            pltpu.VMEM((2, depth, rows, LANES), f32),
            pltpu.VMEM((depth, rows, LANES), f32),
            pltpu.VMEM((depth, rows, LANES), f32),
            pltpu.VMEM((depth + 2, tall, LANES), jnp.int32),
            pltpu.VMEM((depth + 2, tall, LANES), f32),
            pltpu.VMEM((7, depth, rows, LANES), f32),
            pltpu.VMEM((depth, rows, LANES), f32),
            pltpu.VMEM((2, depth, LANES), f32),
            pltpu.VMEM((2, depth, LANES), f32),
            pltpu.VMEM((4, depth, LANES), f32),
            pltpu.VMEM((4, depth, LANES), f32),
            dma((3,)),
            dma((2,)),
            dma((2,)),
            dma((2,)),
            dma((2,)),
            dma((2, chunks)),
            dma((2,)),
            dma((2,)),
            dma((1,)),
            dma((2, chunks)),
            dma((1,)),
            dma((1,)),
            pltpu.SemaphoreType.REGULAR,
            pltpu.SemaphoreType.REGULAR,
        ],
        compiler_params=pltpu.CompilerParams(
            collective_id=0, has_side_effects=True, vmem_limit_bytes=24 * 1024 * 1024
        ),
    )(*[pltpu.with_memory_space_constraint(x, pltpu.HBM) for x in arguments])
    return pl.pallas_call(
        store,
        out_shape=(result, result),
        in_specs=[vmem] * 2,
        out_specs=(hbm, hbm),
        scratch_shapes=[dma((4,))],
        compiler_params=pltpu.CompilerParams(vmem_limit_bytes=1024 * 1024),
    )(*results)


def solution(mesh):
    return jax.shard_map(
        on_device,
        mesh=mesh,
        in_specs=(
            P("space", None, None),
            P("space", None, None),
            P("space", None, None),
            P("node", "space", None, None),
            P("node", "space", None, None),
        ),
        out_specs=(P("node", "space", None, None), P("node", "space", None, None)),
        check_vma=False,
    )
```

```python
import jax
import jax.numpy as jnp
from jax import lax
from jax.experimental import pallas as pl
from jax.experimental.pallas import tpu as pltpu
from jax.sharding import PartitionSpec as P

MESH = pl.DeviceIdType.MESH
LANES = 128
CHUNK = 32
STEP = 16
EDGE = 8

radau_points = (0.08858795951270396, 0.4094668644407347, 0.7876594617608471, 1.0)
time_step = 0.16
onset_level = 0.15
ionic_gain = 8.0
recovery_base = 0.002
recovery_slope = 0.2
recovery_offset = 0.3
conductances = (1.0, 0.35, 0.05)
excitability = (1.0, 0.6, 0.0)


def weight_table():
    table = []
    for target in range(4):
        entries = []
        for column in range(4):
            coeffs = [1.0]
            for other in range(4):
                if other != column:
                    factor = 1.0 / (radau_points[column] - radau_points[other])
                    raised = [0.0] + coeffs
                    lowered = coeffs + [0.0]
                    coeffs = [
                        factor * (raised[place] - radau_points[other] * lowered[place])
                        for place in range(len(raised))
                    ]
            integral = 0.0
            for place in range(len(coeffs)):
                integral = integral + coeffs[place] * radau_points[target] ** (place + 1) / (
                    place + 1
                )
            entries.append(time_step * integral)
        table.append(entries)
    return table


def label_values(labels, values, outside):
    return jnp.where(
        labels == 0,
        jnp.float32(values[0]),
        jnp.where(
            labels == 1,
            jnp.float32(values[1]),
            jnp.where(labels == 2, jnp.float32(values[2]), jnp.float32(outside)),
        ),
    )


def kernel(
    us_hbm,
    vs_hbm,
    lab_hbm,
    ug_hbm,
    vg_hbm,
    out_u,
    out_v,
    u0,
    u1,
    v,
    res,
    us,
    vs,
    lab,
    cond,
    face,
    exc,
    b0s,
    b0r,
    b1s,
    b1r,
    load_sem,
    lab_send,
    lab_recv,
    side_send,
    halo_recv,
    mid_recv,
    row_send,
    row_recv,
    in_send,
    in_recv,
    back_send,
    back_recv,
    hello,
    met,
):
    depth, rows = lab_hbm.shape[0], lab_hbm.shape[1] // 2
    chunks = rows // CHUNK
    node, here = lax.axis_index("node"), lax.axis_index("space")
    count = lax.axis_size("space")
    fold = count // 2
    half = lax.rem(node + here // fold, 2)
    own, other = half * rows, (1 - half) * rows
    has = (here > 0, here < count - 1)
    flips = ((here == fold).astype(jnp.int32), (here == fold - 1).astype(jnp.int32))
    sides = (
        (lax.rem(node + flips[0], 2), here - 1),
        (lax.rem(node + flips[1], 2), here + 1),
    )
    partner = (1 - node, here)
    ours = (1, depth)
    theirs = (depth + 1, 0)

    def mine(k):
        return k * half + (chunks - 1 - k) * (1 - half)

    def its(k):
        return k * (1 - half) + (chunks - 1 - k) * half

    def rows_of(c, base):
        return pl.ds(pl.multiple_of(base + CHUNK * c, 8), CHUNK)

    def step_of(row):
        return pl.ds(pl.multiple_of(row, 8), STEP)

    def remote(src, dst, send, recv, device):
        return pltpu.make_async_remote_copy(
            src_ref=src,
            dst_ref=dst,
            send_sem=send,
            recv_sem=recv,
            device_id=device,
            device_id_type=MESH,
        )

    own_rows = pl.ds(pl.multiple_of(own, 8), rows)
    inner = pl.ds(EDGE, rows)
    slab = pl.ds(1, depth)
    edge_source = pl.ds(pl.multiple_of(rows - EDGE * half, 8), EDGE)
    edge_place = pl.ds(pl.multiple_of((EDGE + rows) * (1 - half), 8), EDGE)
    void_place = pl.ds(pl.multiple_of((EDGE + rows) * half, 8), EDGE)

    def lab_copy(side):
        return remote(
            lab_hbm.at[pl.ds(ours[side] - 1, 1), own_rows],
            lab.at[pl.ds(theirs[side], 1), inner],
            lab_send.at[side],
            lab_recv.at[1 - side],
            sides[side],
        )

    def own_copy(side):
        return remote(
            ug_hbm.at[:, pl.ds(ours[side] - 1, 1), own_rows],
            u0.at[pl.ds(2 * flips[side], 2), pl.ds(theirs[side], 1), inner],
            side_send.at[side],
            halo_recv.at[1 - side],
            sides[side],
        )

    def fwd_copy(side, k):
        at = rows_of(mine(k), EDGE)
        return remote(
            u0.at[pl.ds(2, 2), pl.ds(ours[side], 1), at],
            u0.at[pl.ds(2 - 2 * flips[side], 2), pl.ds(theirs[side], 1), at],
            side_send.at[side],
            halo_recv.at[1 - side],
            sides[side],
        )

    def mid_copy(side, pair, k):
        at = rows_of(mine(k), EDGE)
        to = 2 * (pair + flips[side] - 2 * pair * flips[side])
        return remote(
            u1.at[pl.ds(2 * pair, 2), pl.ds(ours[side], 1), at],
            u1.at[pl.ds(to, 2), pl.ds(theirs[side], 1), at],
            side_send.at[side],
            mid_recv.at[1 - side, k],
            sides[side],
        )

    def in_copy(field, k, c, base):
        return remote(
            (ug_hbm, vg_hbm)[field].at[:, :, rows_of(c, base)],
            (
                u0.at[pl.ds(2, 2), slab, rows_of(c, EDGE)],
                v.at[pl.ds(2, 2), :, rows_of(c, 0)],
            )[field],
            in_send.at[0],
            in_recv.at[field, k],
            partner,
        )

    def sent(field, k):
        return in_copy(field, k, its(k), other)

    def arriving(field, k):
        return in_copy(field, k, mine(k), own)

    def back_copies(row):
        to, full = step_of(row), step_of(own + row)
        return (
            remote(
                res.at[:, :, to],
                out_u.at[:, :, full],
                back_send.at[0],
                back_recv.at[0],
                partner,
            ),
            remote(
                v.at[pl.ds(2, 2), :, to],
                out_v.at[:, :, full],
                back_send.at[0],
                back_recv.at[0],
                partner,
            ),
        )

    row_copies = (
        remote(b0s, b0r, row_send.at[0], row_recv.at[0], partner),
        remote(b1s, b1r, row_send.at[1], row_recv.at[1], partner),
    )

    loads = [
        pltpu.make_async_copy(src, dst, load_sem.at[i])
        for i, src, dst in (
            (0, ug_hbm.at[:, :, own_rows], u0.at[pl.ds(0, 2), slab, inner]),
            (0, ug_hbm.at[:, :, edge_source], u0.at[pl.ds(0, 2), slab, edge_place]),
            (1, lab_hbm.at[:, own_rows], lab.at[slab, inner]),
            (1, lab_hbm.at[:, edge_source], lab.at[slab, edge_place]),
            (2, vg_hbm.at[:, :, own_rows], v.at[pl.ds(0, 2)]),
            (2, us_hbm.at[:, own_rows], us),
            (2, vs_hbm.at[:, own_rows], vs),
        )
    ]
    grown = pl.ds(pl.multiple_of(EDGE * (1 - half), 8), EDGE + rows)

    def await_bytes(ref, sem):
        pltpu.make_async_copy(ref, ref, sem).wait()

    odd, first = here % 2 == 0, node == 1
    host = jnp.logical_and(odd, jnp.logical_not(first))
    guest = jnp.logical_and(odd, first)
    barrier = pltpu.get_barrier_semaphore()

    def signal(sem, device):
        pl.semaphore_signal(sem, inc=1, device_id=device, device_id_type=MESH)

    for copy in loads[:2]:
        copy.start()

    @pl.when(jnp.logical_not(guest))
    def _():
        signal(barrier, partner)

    @pl.when(jnp.logical_not(host))
    def _():
        pl.semaphore_wait(barrier, 1)

    @pl.when(guest)
    def _():
        signal(hello, partner)

    @pl.when(host)
    def _():
        pl.semaphore_wait(hello, 1)

    for k in range(2):
        sent(0, k).start()
    for copy in loads[2:]:
        copy.start()
    for side in (0, 1):

        @pl.when(jnp.logical_and(has[side], jnp.logical_not(jnp.logical_or(odd, sides[side][0] == 1))))
        def _():
            signal(barrier, sides[side])

    def take_row(source, target, nodes):
        line = EDGE + (rows - 1) * (1 - half)

        @pl.loop(0, depth)
        def _(p):
            for j in range(nodes):
                target[j, pl.ds(p, 1)] = source[j, p + 1, pl.ds(line, 1)]

    def put_row(source, target, nodes, first):
        line = EDGE - 1 + (rows + 1) * (1 - half)

        @pl.loop(0, depth)
        def _(p):
            for j in range(nodes):
                target[first(j), p + 1, pl.ds(line, 1)] = source[j, pl.ds(p, 1)]

    await_bytes(u0.at[pl.ds(0, 2), slab, grown], load_sem.at[0])
    take_row(u0, b0s, 2)
    row_copies[0].start()

    @pl.loop(2, chunks)
    def _(k):
        sent(0, k).start()

    @pl.loop(0, chunks)
    def _(k):
        sent(1, k).start()

    beside_count = has[0].astype(jnp.int32) + has[1].astype(jnp.int32)

    @pl.when(host)
    def _():
        pl.semaphore_wait(barrier, beside_count)
        signal(met, partner)

    @pl.when(guest)
    def _():
        pl.semaphore_wait(met, 1)

    for side in (0, 1):

        @pl.when(jnp.logical_and(odd, has[side]))
        def _():
            signal(met, sides[side])

    @pl.when(jnp.logical_not(odd))
    def _():
        pl.semaphore_wait(met, beside_count)

    for side in (0, 1):

        @pl.when(has[side])
        def _():
            lab_copy(side).start()
            own_copy(side).start()

    @pl.loop(0, depth)
    def _(p):
        lab[p + 1, void_place] = jnp.full((EDGE, LANES), 3, jnp.int32)
        for place in range(4):
            u0[place, p + 1, void_place] = jnp.zeros((EDGE, LANES), jnp.float32)
            u1[place, p + 1, void_place] = jnp.zeros((EDGE, LANES), jnp.float32)

    for side in (0, 1):

        @pl.when(jnp.logical_not(has[side]))
        def _():
            plane = (0, depth + 1)[side]

            @pl.loop(0, chunks)
            def _(c):
                at = rows_of(c, EDGE)
                lab[plane, at] = jnp.full((CHUNK, LANES), 3, jnp.int32)
                for place in range(4):
                    u0[place, plane, at] = jnp.zeros((CHUNK, LANES), jnp.float32)
                    u1[place, plane, at] = jnp.zeros((CHUNK, LANES), jnp.float32)

    await_bytes(lab.at[slab, grown], load_sem.at[1])
    for side in (0, 1):

        @pl.when(has[side])
        def _():
            lab_copy(1 - side).wait_recv()

    @pl.loop(0, depth + 2)
    def _(p):
        @pl.loop(0, chunks)
        def _(c):
            at = rows_of(c, EDGE)
            cond[p, at] = label_values(lab[p, at], conductances, 0.0)

    @pl.loop(1, depth + 1)
    def _(p):
        for at in (pl.ds(0, EDGE), pl.ds(EDGE + rows, EDGE)):
            cond[p, at] = label_values(lab[p, at], conductances, 0.0)

    lane = lax.broadcasted_iota(jnp.int32, (STEP, LANES), 1)

    @pl.loop(0, depth)
    def _(p):
        @pl.loop(0, rows // STEP)
        def _(i):
            at, to = step_of(EDGE + STEP * i), step_of(STEP * i)
            row = EDGE + STEP * i
            center = cond[p + 1, at]
            beside = (
                cond[p + 2, at],
                cond[p, at],
                cond[p + 1, pl.ds(row + 1, STEP)],
                cond[p + 1, pl.ds(row - 1, STEP)],
                jnp.where(lane == LANES - 1, 0.0, pltpu.roll(center, LANES - 1, 1)),
                jnp.where(lane == 0, 0.0, pltpu.roll(center, 1, 1)),
            )
            total = jnp.zeros_like(center)
            for f in range(6):
                value = 2.0 * center * beside[f] / (center + beside[f])
                face[f, p, to] = value
                total = total + value
            face[6, p, to] = total
            exc[p, to] = label_values(lab[p + 1, at], excitability, 0.0)

    await_bytes(v, load_sem.at[2])
    row_copies[0].wait_recv()
    put_row(b0r, u0, 2, lambda j: 2 + j)

    @pl.loop(0, chunks)
    def _(k):
        arriving(0, k).wait_recv()
        for side in (0, 1):

            @pl.when(has[side])
            def _():
                fwd_copy(side, k).start()

    for side in (0, 1):

        @pl.when(has[side])
        def _():
            await_bytes(u0.at[:, pl.ds(theirs[1 - side], 1), inner], halo_recv.at[side])

    table = weight_table()
    weights = [
        [
            jnp.where(
                node == 0,
                jnp.float32(table[m][j]),
                jnp.float32(table[(m + 2) % 4][(j + 2) % 4]),
            )
            for j in range(4)
        ]
        for m in range(4)
    ]

    def sweep(source, start, steps, write):
        @pl.loop(0, depth * steps)
        def _(i):
            p, first = i % depth, start + STEP * (i // depth)
            at, to = step_of(EDGE + first), step_of(first)
            row = EDGE + first
            faces = [face[f, p, to] for f in range(7)]
            excite = exc[p, to]
            sum_u = [us[p, to]] * 4
            sum_v = [vs[p, to]] * 4
            for j in range(4):
                mid = source[j, p + 1, at]
                v_mid = v[j, p, to]
                spread = (
                    faces[0] * source[j, p + 2, at]
                    + faces[1] * source[j, p, at]
                    + faces[2] * source[j, p + 1, pl.ds(row + 1, STEP)]
                    + faces[3] * source[j, p + 1, pl.ds(row - 1, STEP)]
                    + faces[4] * pltpu.roll(mid, LANES - 1, 1)
                    + faces[5] * pltpu.roll(mid, 1, 1)
                )
                scaled = ionic_gain * mid
                growth = (scaled - ionic_gain * onset_level) * (1.0 - mid) - v_mid
                rate_u = spread + mid * (excite * growth - faces[6])
                recovery = recovery_base + recovery_slope * v_mid / jnp.maximum(
                    mid + recovery_offset, recovery_offset
                )
                rate_v = recovery * (-v_mid - scaled * (mid - (onset_level + 1.0)))
                for m in range(4):
                    sum_u[m] = sum_u[m] + weights[m][j] * rate_u
                    sum_v[m] = sum_v[m] + weights[m][j] * rate_v
            write(p, first, sum_u, sum_v)

    def first_sweep(k):
        def write(p, first, new_u, new_v):
            at, to = step_of(EDGE + first), step_of(first)
            for m in range(4):
                u1[m, p + 1, at] = new_u[m]
                v[m, p, to] = new_v[m]

        sweep(u0, CHUNK * mine(k), CHUNK // STEP, write)

    def second_sweep(row):
        def write(p, first, new_u, new_v):
            to, full = step_of(first), step_of(own + first)
            for m in range(2):
                out_u[m, p, full] = new_u[m]
                out_v[m, p, full] = new_v[m]
                res[m, p, to] = new_u[2 + m]
                v[2 + m, p, to] = new_v[2 + m]

        sweep(u1, row, 1, write)
        for copy in back_copies(row):
            copy.start()

    def await_mid(k):
        at = rows_of(mine(k), EDGE)
        for side in (0, 1):

            @pl.when(has[side])
            def _():
                await_bytes(u1.at[:, pl.ds(theirs[1 - side], 1), at], mid_recv.at[side, k])

    each = CHUNK // STEP
    steps = chunks * each

    @pl.loop(0, chunks + 1)
    def _(k):
        @pl.when(k < chunks)
        def _():
            arriving(1, k).wait_recv()
            first_sweep(k)
            for side in (0, 1):

                @pl.when(has[side])
                def _():
                    for pair in (0, 1):
                        mid_copy(side, pair, k).start()

        @pl.when(k == 0)
        def _():
            take_row(u1, b1s, 4)
            row_copies[1].start()

        @pl.when(k == 1)
        def _():
            await_mid(0)

        @pl.when(jnp.logical_and(k > 0, k < chunks))
        def _():
            await_mid(k)

        @pl.when(k == chunks)
        def _():
            row_copies[1].wait_recv()
            put_row(b1r, u1, 4, lambda j: (j + 2) % 4)

        @pl.when(k > 0)
        def _():
            @pl.loop(0, each)
            def _(i):
                t = lax.rem(each * (k - 1) + 1 + i, steps)
                second_sweep(STEP * (t * half + (steps - 1 - t) * (1 - half)))

    for side in (0, 1):

        @pl.when(has[side])
        def _():
            lab_copy(side).wait_send()
            await_bytes(u1.at[:, pl.ds(0, 2), inner], side_send.at[side])

    for copy in row_copies:
        copy.wait_send()
    await_bytes(v, in_send.at[0])
    await_bytes(v, back_send.at[0])
    await_bytes(v, back_recv.at[0])


def store(u_vmem, v_vmem, u_hbm, v_hbm, sem):
    copies = [
        pltpu.make_async_copy(src.at[m, p], dst.at[m, p], sem.at[2 * i + m])
        for i, (src, dst) in enumerate(((u_vmem, u_hbm), (v_vmem, v_hbm)))
        for m in range(2)
        for p in range(u_vmem.shape[1])
    ]
    for copy in copies:
        copy.start()
    for copy in copies:
        copy.wait()


def on_device(*arguments):
    labels = arguments[2]
    depth, width = labels.shape[0], labels.shape[1]
    rows = width // 2
    chunks = rows // CHUNK
    tall = rows + 2 * EDGE
    f32 = jnp.float32
    hbm = pl.BlockSpec(memory_space=pltpu.HBM)
    vmem = pl.BlockSpec(memory_space=pltpu.VMEM)
    dma = pltpu.SemaphoreType.DMA
    result = jax.ShapeDtypeStruct((2, depth, width, LANES), f32)
    results = pl.pallas_call(
        kernel,
        out_shape=(result, result),
        in_specs=[hbm] * 5,
        out_specs=(vmem, vmem),
        scratch_shapes=[
            pltpu.VMEM((4, depth + 2, tall, LANES), f32),
            pltpu.VMEM((4, depth + 2, tall, LANES), f32),
            pltpu.VMEM((4, depth, rows, LANES), f32),
            pltpu.VMEM((2, depth, rows, LANES), f32),
            pltpu.VMEM((depth, rows, LANES), f32),
            pltpu.VMEM((depth, rows, LANES), f32),
            pltpu.VMEM((depth + 2, tall, LANES), jnp.int32),
            pltpu.VMEM((depth + 2, tall, LANES), f32),
            pltpu.VMEM((7, depth, rows, LANES), f32),
            pltpu.VMEM((depth, rows, LANES), f32),
            pltpu.VMEM((2, depth, LANES), f32),
            pltpu.VMEM((2, depth, LANES), f32),
            pltpu.VMEM((4, depth, LANES), f32),
            pltpu.VMEM((4, depth, LANES), f32),
            dma((3,)),
            dma((2,)),
            dma((2,)),
            dma((2,)),
            dma((2,)),
            dma((2, chunks)),
            dma((2,)),
            dma((2,)),
            dma((1,)),
            dma((2, chunks)),
            dma((1,)),
            dma((1,)),
            pltpu.SemaphoreType.REGULAR,
            pltpu.SemaphoreType.REGULAR,
        ],
        compiler_params=pltpu.CompilerParams(
            collective_id=0, has_side_effects=True, vmem_limit_bytes=24 * 1024 * 1024
        ),
    )(*[pltpu.with_memory_space_constraint(x, pltpu.HBM) for x in arguments])
    return pl.pallas_call(
        store,
        out_shape=(result, result),
        in_specs=[vmem] * 2,
        out_specs=(hbm, hbm),
        scratch_shapes=[dma((4,))],
        compiler_params=pltpu.CompilerParams(vmem_limit_bytes=1024 * 1024),
    )(*results)


def solution(mesh):
    return jax.shard_map(
        on_device,
        mesh=mesh,
        in_specs=(
            P("space", None, None),
            P("space", None, None),
            P("space", None, None),
            P("node", "space", None, None),
            P("node", "space", None, None),
        ),
        out_specs=(P("node", "space", None, None), P("node", "space", None, None)),
        check_vma=False,
    )
```

```python
import jax
import jax.numpy as jnp
from jax import lax
from jax.experimental import pallas as pl
from jax.experimental.pallas import tpu as pltpu
from jax.sharding import PartitionSpec as P

MESH = pl.DeviceIdType.MESH
LANES = 128
CHUNK = 32
STEP = 16
EDGE = 8

radau_points = (0.08858795951270396, 0.4094668644407347, 0.7876594617608471, 1.0)
time_step = 0.16
onset_level = 0.15
ionic_gain = 8.0
recovery_base = 0.002
recovery_slope = 0.2
recovery_offset = 0.3
conductances = (1.0, 0.35, 0.05)
excitability = (1.0, 0.6, 0.0)


def weight_table():
    table = []
    for target in range(4):
        entries = []
        for column in range(4):
            coeffs = [1.0]
            for other in range(4):
                if other != column:
                    factor = 1.0 / (radau_points[column] - radau_points[other])
                    raised = [0.0] + coeffs
                    lowered = coeffs + [0.0]
                    coeffs = [
                        factor * (raised[place] - radau_points[other] * lowered[place])
                        for place in range(len(raised))
                    ]
            integral = 0.0
            for place in range(len(coeffs)):
                integral = integral + coeffs[place] * radau_points[target] ** (place + 1) / (
                    place + 1
                )
            entries.append(time_step * integral)
        table.append(entries)
    return table


def label_values(labels, values, outside):
    return jnp.where(
        labels == 0,
        jnp.float32(values[0]),
        jnp.where(
            labels == 1,
            jnp.float32(values[1]),
            jnp.where(labels == 2, jnp.float32(values[2]), jnp.float32(outside)),
        ),
    )


def kernel(
    us_hbm,
    vs_hbm,
    lab_hbm,
    ug_hbm,
    vg_hbm,
    out_u,
    out_v,
    u0,
    u1,
    v,
    res,
    us,
    vs,
    lab,
    cond,
    face,
    exc,
    lines,
    b0r,
    b1r,
    load_sem,
    side_send,
    halo_recv,
    mid_recv,
    row_send,
    row_recv,
    in_send,
    in_recv,
    back_send,
    back_recv,
    hello,
    met,
):
    depth, rows = lab_hbm.shape[0], lab_hbm.shape[1] // 2
    chunks = rows // CHUNK
    node, here = lax.axis_index("node"), lax.axis_index("space")
    count = lax.axis_size("space")
    fold = count // 2
    half = lax.rem(node + here // fold, 2)
    own, other = half * rows, (1 - half) * rows
    has = (here > 0, here < count - 1)
    flips = ((here == fold).astype(jnp.int32), (here == fold - 1).astype(jnp.int32))
    sides = (
        (lax.rem(node + flips[0], 2), here - 1),
        (lax.rem(node + flips[1], 2), here + 1),
    )
    partner = (1 - node, here)
    ours = (1, depth)
    theirs = (depth + 1, 0)

    def mine(k):
        return k * half + (chunks - 1 - k) * (1 - half)

    def its(k):
        return k * (1 - half) + (chunks - 1 - k) * half

    def rows_of(c, base):
        return pl.ds(pl.multiple_of(base + CHUNK * c, 8), CHUNK)

    def step_of(row):
        return pl.ds(pl.multiple_of(row, 8), STEP)

    def remote(src, dst, send, recv, device):
        return pltpu.make_async_remote_copy(
            src_ref=src,
            dst_ref=dst,
            send_sem=send,
            recv_sem=recv,
            device_id=device,
            device_id_type=MESH,
        )

    own_rows = pl.ds(pl.multiple_of(own, 8), rows)
    inner = pl.ds(EDGE, rows)
    slab = pl.ds(1, depth)
    edge_source = pl.ds(pl.multiple_of(rows - EDGE * half, 8), EDGE)
    edge_place = pl.ds(pl.multiple_of((EDGE + rows) * (1 - half), 8), EDGE)
    void_place = pl.ds(pl.multiple_of((EDGE + rows) * half, 8), EDGE)

    def lab_copy(side):
        return remote(
            lab_hbm.at[pl.ds(ours[side] - 1, 1), own_rows],
            lab.at[pl.ds(theirs[side], 1), inner],
            side_send.at[0],
            halo_recv.at[0],
            sides[side],
        )

    def own_copy(side):
        return remote(
            ug_hbm.at[:, pl.ds(ours[side] - 1, 1), own_rows],
            u0.at[pl.ds(2 * flips[side], 2), pl.ds(theirs[side], 1), inner],
            side_send.at[0],
            halo_recv.at[0],
            sides[side],
        )

    def fwd_copy(side):
        return remote(
            u0.at[pl.ds(2, 2), pl.ds(ours[side], 1), inner],
            u0.at[pl.ds(2 - 2 * flips[side], 2), pl.ds(theirs[side], 1), inner],
            side_send.at[0],
            halo_recv.at[0],
            sides[side],
        )

    def mid_copy(side, pair, k):
        at = rows_of(mine(k), EDGE)
        to = 2 * (pair + flips[side] - 2 * pair * flips[side])
        return remote(
            u1.at[pl.ds(2 * pair, 2), pl.ds(ours[side], 1), at],
            u1.at[pl.ds(to, 2), pl.ds(theirs[side], 1), at],
            side_send.at[0],
            mid_recv.at[k],
            sides[side],
        )

    def in_copy(field, k, c, base):
        return remote(
            (ug_hbm, vg_hbm)[field].at[:, :, rows_of(c, base)],
            (
                u0.at[pl.ds(2, 2), slab, rows_of(c, EDGE)],
                v.at[pl.ds(2, 2), :, rows_of(c, 0)],
            )[field],
            in_send.at[0],
            in_recv.at[k if field else chunks],
            partner,
        )

    def sent(field, k):
        return in_copy(field, k, its(k), other)

    def arriving(field, k):
        return in_copy(field, k, mine(k), own)

    def back_copies(row):
        to, full = step_of(row), step_of(own + row)
        return (
            remote(
                res.at[:, :, to],
                out_u.at[:, :, full],
                back_send.at[0],
                back_recv.at[0],
                partner,
            ),
            remote(
                v.at[pl.ds(2, 2), :, to],
                out_v.at[:, :, full],
                back_send.at[0],
                back_recv.at[0],
                partner,
            ),
        )

    row_copies = (
        remote(lines.at[pl.ds(0, 2)], b0r, row_send.at[0], row_recv.at[0], partner),
        remote(lines.at[pl.ds(2, 4)], b1r, row_send.at[0], row_recv.at[1], partner),
    )

    loads = [
        pltpu.make_async_copy(src, dst, load_sem.at[i])
        for i, src, dst in (
            (0, ug_hbm.at[:, :, own_rows], u0.at[pl.ds(0, 2), slab, inner]),
            (0, ug_hbm.at[:, :, edge_source], u0.at[pl.ds(0, 2), slab, edge_place]),
            (1, lab_hbm.at[:, own_rows], lab.at[slab, inner]),
            (1, lab_hbm.at[:, edge_source], lab.at[slab, edge_place]),
            (2, vg_hbm.at[:, :, own_rows], v.at[pl.ds(0, 2)]),
            (2, us_hbm.at[:, own_rows], us),
            (2, vs_hbm.at[:, own_rows], vs),
        )
    ]
    grown = pl.ds(pl.multiple_of(EDGE * (1 - half), 8), EDGE + rows)

    def await_bytes(ref, sem):
        pltpu.make_async_copy(ref, ref, sem).wait()

    both = jnp.logical_and(has[0], has[1])

    def await_sides(few, all_of_them, sem):
        @pl.when(both)
        def _():
            await_bytes(all_of_them, sem)

        @pl.when(jnp.logical_not(both))
        def _():
            await_bytes(few, sem)

    odd, first = here % 2 == 0, node == 1
    host = jnp.logical_and(odd, jnp.logical_not(first))
    guest = jnp.logical_and(odd, first)
    barrier = pltpu.get_barrier_semaphore()

    def signal(sem, device):
        pl.semaphore_signal(sem, inc=1, device_id=device, device_id_type=MESH)

    for copy in loads[:2]:
        copy.start()

    @pl.when(jnp.logical_not(guest))
    def _():
        signal(barrier, partner)

    @pl.when(jnp.logical_not(host))
    def _():
        pl.semaphore_wait(barrier, 1)

    @pl.when(guest)
    def _():
        signal(hello, partner)

    @pl.when(host)
    def _():
        pl.semaphore_wait(hello, 1)

    for k in range(2):
        sent(0, k).start()
    for copy in loads[2:]:
        copy.start()
    for side in (0, 1):

        @pl.when(jnp.logical_and(has[side], jnp.logical_not(jnp.logical_or(odd, sides[side][0] == 1))))
        def _():
            signal(barrier, sides[side])

    def take_row(source, place, nodes):
        line = EDGE + (rows - 1) * (1 - half)

        @pl.loop(0, depth)
        def _(p):
            for j in range(nodes):
                lines[place + j, pl.ds(p, 1)] = source[j, p + 1, pl.ds(line, 1)]

    def put_row(source, target, nodes, first):
        line = EDGE - 1 + (rows + 1) * (1 - half)

        @pl.loop(0, depth)
        def _(p):
            for j in range(nodes):
                target[first(j), p + 1, pl.ds(line, 1)] = source[j, pl.ds(p, 1)]

    await_bytes(u0.at[pl.ds(0, 2), slab, grown], load_sem.at[0])
    take_row(u0, 0, 2)
    row_copies[0].start()

    @pl.loop(2, chunks)
    def _(k):
        sent(0, k).start()

    @pl.loop(0, chunks)
    def _(k):
        sent(1, k).start()

    beside_count = has[0].astype(jnp.int32) + has[1].astype(jnp.int32)

    @pl.when(host)
    def _():
        pl.semaphore_wait(barrier, beside_count)
        signal(met, partner)

    @pl.when(guest)
    def _():
        pl.semaphore_wait(met, 1)

    for side in (0, 1):

        @pl.when(jnp.logical_and(odd, has[side]))
        def _():
            signal(met, sides[side])

    @pl.when(jnp.logical_not(odd))
    def _():
        pl.semaphore_wait(met, beside_count)

    for side in (0, 1):

        @pl.when(has[side])
        def _():
            lab_copy(side).start()
            own_copy(side).start()

    @pl.loop(0, depth)
    def _(p):
        lab[p + 1, void_place] = jnp.full((EDGE, LANES), 3, jnp.int32)
        for place in range(4):
            u0[place, p + 1, void_place] = jnp.zeros((EDGE, LANES), jnp.float32)
            u1[place, p + 1, void_place] = jnp.zeros((EDGE, LANES), jnp.float32)

    for side in (0, 1):

        @pl.when(jnp.logical_not(has[side]))
        def _():
            plane = (0, depth + 1)[side]

            @pl.loop(0, chunks)
            def _(c):
                at = rows_of(c, EDGE)
                lab[plane, at] = jnp.full((CHUNK, LANES), 3, jnp.int32)
                for place in range(4):
                    u0[place, plane, at] = jnp.zeros((CHUNK, LANES), jnp.float32)
                    u1[place, plane, at] = jnp.zeros((CHUNK, LANES), jnp.float32)

    await_bytes(v, load_sem.at[2])
    row_copies[0].wait_recv()
    put_row(b0r, u0, 2, lambda j: 2 + j)

    await_bytes(u0.at[pl.ds(2, 2), slab, inner], in_recv.at[chunks])
    for side in (0, 1):

        @pl.when(has[side])
        def _():
            fwd_copy(side).start()

    await_sides(
        u1.at[0, pl.ds(0, 5), inner], u1.at[0, pl.ds(0, 10), inner], halo_recv.at[0]
    )

    await_bytes(lab.at[slab, grown], load_sem.at[1])

    @pl.loop(0, depth + 2)
    def _(p):
        @pl.loop(0, chunks)
        def _(c):
            at = rows_of(c, EDGE)
            cond[p, at] = label_values(lab[p, at], conductances, 0.0)

    @pl.loop(1, depth + 1)
    def _(p):
        for at in (pl.ds(0, EDGE), pl.ds(EDGE + rows, EDGE)):
            cond[p, at] = label_values(lab[p, at], conductances, 0.0)

    lane = lax.broadcasted_iota(jnp.int32, (STEP, LANES), 1)

    @pl.loop(0, depth)
    def _(p):
        @pl.loop(0, rows // STEP)
        def _(i):
            at, to = step_of(EDGE + STEP * i), step_of(STEP * i)
            row = EDGE + STEP * i
            center = cond[p + 1, at]
            beside = (
                cond[p + 2, at],
                cond[p, at],
                cond[p + 1, pl.ds(row + 1, STEP)],
                cond[p + 1, pl.ds(row - 1, STEP)],
                jnp.where(lane == LANES - 1, 0.0, pltpu.roll(center, LANES - 1, 1)),
                jnp.where(lane == 0, 0.0, pltpu.roll(center, 1, 1)),
            )
            total = jnp.zeros_like(center)
            for f in range(6):
                value = 2.0 * center * beside[f] / (center + beside[f])
                face[f, p, to] = value
                total = total + value
            face[6, p, to] = total
            exc[p, to] = label_values(lab[p + 1, at], excitability, 0.0)

    table = weight_table()
    weights = [
        [
            jnp.where(
                node == 0,
                jnp.float32(table[m][j]),
                jnp.float32(table[(m + 2) % 4][(j + 2) % 4]),
            )
            for j in range(4)
        ]
        for m in range(4)
    ]

    def sweep(source, start, steps, write):
        @pl.loop(0, depth * steps)
        def _(i):
            p, first = i % depth, start + STEP * (i // depth)
            at, to = step_of(EDGE + first), step_of(first)
            row = EDGE + first
            faces = [face[f, p, to] for f in range(7)]
            excite = exc[p, to]
            sum_u = [us[p, to]] * 4
            sum_v = [vs[p, to]] * 4
            for j in range(4):
                mid = source[j, p + 1, at]
                v_mid = v[j, p, to]
                spread = (
                    faces[0] * source[j, p + 2, at]
                    + faces[1] * source[j, p, at]
                    + faces[2] * source[j, p + 1, pl.ds(row + 1, STEP)]
                    + faces[3] * source[j, p + 1, pl.ds(row - 1, STEP)]
                    + faces[4] * pltpu.roll(mid, LANES - 1, 1)
                    + faces[5] * pltpu.roll(mid, 1, 1)
                )
                scaled = ionic_gain * mid
                growth = (scaled - ionic_gain * onset_level) * (1.0 - mid) - v_mid
                rate_u = spread + mid * (excite * growth - faces[6])
                recovery = recovery_base + recovery_slope * v_mid / jnp.maximum(
                    mid + recovery_offset, recovery_offset
                )
                rate_v = recovery * (-v_mid - scaled * (mid - (onset_level + 1.0)))
                for m in range(4):
                    sum_u[m] = sum_u[m] + weights[m][j] * rate_u
                    sum_v[m] = sum_v[m] + weights[m][j] * rate_v
            write(p, first, sum_u, sum_v)

    def first_sweep(k):
        def write(p, first, new_u, new_v):
            at, to = step_of(EDGE + first), step_of(first)
            for m in range(4):
                u1[m, p + 1, at] = new_u[m]
                v[m, p, to] = new_v[m]

        sweep(u0, CHUNK * mine(k), CHUNK // STEP, write)

    def second_sweep(row):
        def write(p, first, new_u, new_v):
            to, full = step_of(first), step_of(own + first)
            for m in range(2):
                out_u[m, p, full] = new_u[m]
                out_v[m, p, full] = new_v[m]
                res[m, p, to] = new_u[2 + m]
                v[2 + m, p, to] = new_v[2 + m]

        sweep(u1, row, 1, write)
        for copy in back_copies(row):
            copy.start()

    def await_mid(k):
        at = rows_of(mine(k), EDGE)
        await_sides(u1.at[:, pl.ds(0, 1), at], u1.at[:, pl.ds(0, 2), at], mid_recv.at[k])

    each = CHUNK // STEP
    steps = chunks * each

    @pl.loop(0, chunks + 1)
    def _(k):
        @pl.when(k < chunks)
        def _():
            arriving(1, k).wait_recv()
            first_sweep(k)
            for side in (0, 1):

                @pl.when(has[side])
                def _():
                    for pair in (0, 1):
                        mid_copy(side, pair, k).start()

        @pl.when(k == 0)
        def _():
            take_row(u1, 2, 4)
            row_copies[1].start()

        @pl.when(k == 1)
        def _():
            await_mid(0)

        @pl.when(jnp.logical_and(k > 0, k < chunks))
        def _():
            await_mid(k)

        @pl.when(k == chunks)
        def _():
            row_copies[1].wait_recv()
            put_row(b1r, u1, 4, lambda j: (j + 2) % 4)

        @pl.when(k > 0)
        def _():
            @pl.loop(0, each)
            def _(i):
                t = lax.rem(each * (k - 1) + 1 + i, steps)
                second_sweep(STEP * (t * half + (steps - 1 - t) * (1 - half)))

    await_sides(
        u1.at[0, pl.ds(0, 9), inner], u1.at[pl.ds(0, 2), pl.ds(0, 9), inner], side_send.at[0]
    )
    await_bytes(lines, row_send.at[0])
    await_bytes(v, in_send.at[0])
    await_bytes(v, back_send.at[0])
    await_bytes(v, back_recv.at[0])


def store(u_vmem, v_vmem, u_hbm, v_hbm, sem):
    pairs = ((u_vmem, u_hbm), (v_vmem, v_hbm))
    for i, (src, dst) in enumerate(pairs):
        for m in range(2):
            for p in range(u_vmem.shape[1]):
                pltpu.make_async_copy(src.at[m, p], dst.at[m, p], sem.at[i]).start()
    for i, (src, dst) in enumerate(pairs):
        pltpu.make_async_copy(src, dst, sem.at[i]).wait()


def on_device(*arguments):
    labels = arguments[2]
    depth, width = labels.shape[0], labels.shape[1]
    rows = width // 2
    chunks = rows // CHUNK
    tall = rows + 2 * EDGE
    f32 = jnp.float32
    hbm = pl.BlockSpec(memory_space=pltpu.HBM)
    vmem = pl.BlockSpec(memory_space=pltpu.VMEM)
    dma = pltpu.SemaphoreType.DMA
    result = jax.ShapeDtypeStruct((2, depth, width, LANES), f32)
    results = pl.pallas_call(
        kernel,
        out_shape=(result, result),
        in_specs=[hbm] * 5,
        out_specs=(vmem, vmem),
        scratch_shapes=[
            pltpu.VMEM((4, depth + 2, tall, LANES), f32),
            pltpu.VMEM((4, depth + 2, tall, LANES), f32),
            pltpu.VMEM((4, depth, rows, LANES), f32),
            pltpu.VMEM((2, depth, rows, LANES), f32),
            pltpu.VMEM((depth, rows, LANES), f32),
            pltpu.VMEM((depth, rows, LANES), f32),
            pltpu.VMEM((depth + 2, tall, LANES), jnp.int32),
            pltpu.VMEM((depth + 2, tall, LANES), f32),
            pltpu.VMEM((7, depth, rows, LANES), f32),
            pltpu.VMEM((depth, rows, LANES), f32),
            pltpu.VMEM((6, depth, LANES), f32),
            pltpu.VMEM((2, depth, LANES), f32),
            pltpu.VMEM((4, depth, LANES), f32),
            dma((3,)),
            dma((1,)),
            dma((1,)),
            dma((chunks,)),
            dma((1,)),
            dma((2,)),
            dma((1,)),
            dma((chunks + 1,)),
            dma((1,)),
            dma((1,)),
            pltpu.SemaphoreType.REGULAR,
            pltpu.SemaphoreType.REGULAR,
        ],
        compiler_params=pltpu.CompilerParams(
            collective_id=0, has_side_effects=True, vmem_limit_bytes=24 * 1024 * 1024
        ),
    )(*[pltpu.with_memory_space_constraint(x, pltpu.HBM) for x in arguments])
    return pl.pallas_call(
        store,
        out_shape=(result, result),
        in_specs=[vmem] * 2,
        out_specs=(hbm, hbm),
        scratch_shapes=[dma((2,))],
        compiler_params=pltpu.CompilerParams(vmem_limit_bytes=1024 * 1024),
    )(*results)


def solution(mesh):
    return jax.shard_map(
        on_device,
        mesh=mesh,
        in_specs=(
            P("space", None, None),
            P("space", None, None),
            P("space", None, None),
            P("node", "space", None, None),
            P("node", "space", None, None),
        ),
        out_specs=(P("node", "space", None, None), P("node", "space", None, None)),
        check_vma=False,
    )
```

```python
import jax
import jax.numpy as jnp
from jax import lax
from jax.experimental import pallas as pl
from jax.experimental.pallas import tpu as pltpu
from jax.sharding import PartitionSpec as P

MESH = pl.DeviceIdType.MESH
LANES = 128
CHUNK = 32
STEP = 16
EDGE = 8

radau_points = (0.08858795951270396, 0.4094668644407347, 0.7876594617608471, 1.0)
time_step = 0.16
onset_level = 0.15
ionic_gain = 8.0
recovery_base = 0.002
recovery_slope = 0.2
recovery_offset = 0.3
conductances = (1.0, 0.35, 0.05)
excitability = (1.0, 0.6, 0.0)


def weight_table():
    table = []
    for target in range(4):
        entries = []
        for column in range(4):
            coeffs = [1.0]
            for other in range(4):
                if other != column:
                    factor = 1.0 / (radau_points[column] - radau_points[other])
                    raised = [0.0] + coeffs
                    lowered = coeffs + [0.0]
                    coeffs = [
                        factor * (raised[place] - radau_points[other] * lowered[place])
                        for place in range(len(raised))
                    ]
            integral = 0.0
            for place in range(len(coeffs)):
                integral = integral + coeffs[place] * radau_points[target] ** (place + 1) / (
                    place + 1
                )
            entries.append(time_step * integral)
        table.append(entries)
    return table


def label_values(labels, values, outside):
    return jnp.where(
        labels == 0,
        jnp.float32(values[0]),
        jnp.where(
            labels == 1,
            jnp.float32(values[1]),
            jnp.where(labels == 2, jnp.float32(values[2]), jnp.float32(outside)),
        ),
    )


def kernel(
    us_hbm,
    vs_hbm,
    lab_hbm,
    ug_hbm,
    vg_hbm,
    out_u,
    out_v,
    u0,
    u1,
    v,
    res,
    us,
    vs,
    lab,
    cond,
    face,
    exc,
    lines,
    b0r,
    b1r,
    load_sem,
    side_send,
    halo_recv,
    mid_recv,
    row_send,
    row_recv,
    in_send,
    in_recv,
    back_send,
    back_recv,
    hello,
    met,
):
    depth, rows = lab_hbm.shape[0], lab_hbm.shape[1] // 2
    chunks = rows // CHUNK
    node, here = lax.axis_index("node"), lax.axis_index("space")
    count = lax.axis_size("space")
    fold = count // 2
    half = lax.rem(node + here // fold, 2)
    own, other = half * rows, (1 - half) * rows
    has = (here > 0, here < count - 1)
    flips = ((here == fold).astype(jnp.int32), (here == fold - 1).astype(jnp.int32))
    sides = (
        (lax.rem(node + flips[0], 2), here - 1),
        (lax.rem(node + flips[1], 2), here + 1),
    )
    partner = (1 - node, here)
    ours = (1, depth)
    theirs = (depth + 1, 0)

    def mine(k):
        return k * half + (chunks - 1 - k) * (1 - half)

    def its(k):
        return k * (1 - half) + (chunks - 1 - k) * half

    def rows_of(c, base):
        return pl.ds(pl.multiple_of(base + CHUNK * c, 8), CHUNK)

    def step_of(row):
        return pl.ds(pl.multiple_of(row, 8), STEP)

    def remote(src, dst, send, recv, device):
        return pltpu.make_async_remote_copy(
            src_ref=src,
            dst_ref=dst,
            send_sem=send,
            recv_sem=recv,
            device_id=device,
            device_id_type=MESH,
        )

    own_rows = pl.ds(pl.multiple_of(own, 8), rows)
    inner = pl.ds(EDGE, rows)
    slab = pl.ds(1, depth)
    edge_source = pl.ds(pl.multiple_of(rows - EDGE * half, 8), EDGE)
    edge_place = pl.ds(pl.multiple_of((EDGE + rows) * (1 - half), 8), EDGE)
    void_place = pl.ds(pl.multiple_of((EDGE + rows) * half, 8), EDGE)

    def lab_copy(side):
        return remote(
            lab_hbm.at[pl.ds(ours[side] - 1, 1), own_rows],
            lab.at[pl.ds(theirs[side], 1), inner],
            side_send.at[0],
            halo_recv.at[0],
            sides[side],
        )

    def own_copy(side):
        return remote(
            ug_hbm.at[:, pl.ds(ours[side] - 1, 1), own_rows],
            u0.at[pl.ds(2 * flips[side], 2), pl.ds(theirs[side], 1), inner],
            side_send.at[0],
            halo_recv.at[0],
            sides[side],
        )

    def fwd_copy(side):
        return remote(
            u0.at[pl.ds(2, 2), pl.ds(ours[side], 1), inner],
            u0.at[pl.ds(2 - 2 * flips[side], 2), pl.ds(theirs[side], 1), inner],
            side_send.at[0],
            halo_recv.at[0],
            sides[side],
        )

    def mid_copy(side, pair, k):
        at = rows_of(mine(k), EDGE)
        to = 2 * (pair + flips[side] - 2 * pair * flips[side])
        return remote(
            u1.at[pl.ds(2 * pair, 2), pl.ds(ours[side], 1), at],
            u1.at[pl.ds(to, 2), pl.ds(theirs[side], 1), at],
            side_send.at[0],
            mid_recv.at[k],
            sides[side],
        )

    def in_copy(field, k, c, base):
        return remote(
            (ug_hbm, vg_hbm)[field].at[:, :, rows_of(c, base)],
            (
                u0.at[pl.ds(2, 2), slab, rows_of(c, EDGE)],
                v.at[pl.ds(2, 2), :, rows_of(c, 0)],
            )[field],
            in_send.at[0],
            in_recv.at[k if field else chunks],
            partner,
        )

    def sent(field, k):
        return in_copy(field, k, its(k), other)

    def arriving(field, k):
        return in_copy(field, k, mine(k), own)

    def back_copies(row):
        to, full = step_of(row), step_of(own + row)
        return (
            remote(
                res.at[:, :, to],
                out_u.at[:, :, full],
                back_send.at[0],
                back_recv.at[0],
                partner,
            ),
            remote(
                v.at[pl.ds(2, 2), :, to],
                out_v.at[:, :, full],
                back_send.at[0],
                back_recv.at[0],
                partner,
            ),
        )

    row_copies = (
        remote(lines.at[pl.ds(0, 2)], b0r, row_send.at[0], row_recv.at[0], partner),
        remote(lines.at[pl.ds(2, 4)], b1r, row_send.at[0], row_recv.at[1], partner),
    )

    loads = [
        pltpu.make_async_copy(src, dst, load_sem.at[i])
        for i, src, dst in (
            (0, ug_hbm.at[:, :, own_rows], u0.at[pl.ds(0, 2), slab, inner]),
            (0, ug_hbm.at[:, :, edge_source], u0.at[pl.ds(0, 2), slab, edge_place]),
            (1, lab_hbm.at[:, own_rows], lab.at[slab, inner]),
            (1, lab_hbm.at[:, edge_source], lab.at[slab, edge_place]),
            (2, vg_hbm.at[:, :, own_rows], v.at[pl.ds(0, 2)]),
            (2, us_hbm.at[:, own_rows], us),
            (2, vs_hbm.at[:, own_rows], vs),
        )
    ]
    grown = pl.ds(pl.multiple_of(EDGE * (1 - half), 8), EDGE + rows)

    def await_bytes(ref, sem):
        pltpu.make_async_copy(ref, ref, sem).wait()

    both = jnp.logical_and(has[0], has[1])

    def await_sides(few, all_of_them, sem):
        @pl.when(both)
        def _():
            await_bytes(all_of_them, sem)

        @pl.when(jnp.logical_not(both))
        def _():
            await_bytes(few, sem)

    odd, first = here % 2 == 0, node == 1
    host = jnp.logical_and(odd, jnp.logical_not(first))
    guest = jnp.logical_and(odd, first)
    barrier = pltpu.get_barrier_semaphore()

    def signal(sem, device):
        pl.semaphore_signal(sem, inc=1, device_id=device, device_id_type=MESH)

    @pl.when(jnp.logical_not(guest))
    def _():
        signal(barrier, partner)

    @pl.when(jnp.logical_not(host))
    def _():
        pl.semaphore_wait(barrier, 1)

    @pl.when(guest)
    def _():
        signal(hello, partner)

    @pl.when(host)
    def _():
        pl.semaphore_wait(hello, 1)

    for k in range(2):
        sent(0, k).start()
    for copy in loads:
        copy.start()
    for side in (0, 1):

        @pl.when(jnp.logical_and(has[side], jnp.logical_not(jnp.logical_or(odd, sides[side][0] == 1))))
        def _():
            signal(barrier, sides[side])

    def take_row(source, place, nodes):
        line = EDGE + (rows - 1) * (1 - half)

        @pl.loop(0, depth)
        def _(p):
            for j in range(nodes):
                lines[place + j, pl.ds(p, 1)] = source[j, p + 1, pl.ds(line, 1)]

    def put_row(source, target, nodes, first):
        line = EDGE - 1 + (rows + 1) * (1 - half)

        @pl.loop(0, depth)
        def _(p):
            for j in range(nodes):
                target[first(j), p + 1, pl.ds(line, 1)] = source[j, pl.ds(p, 1)]

    await_bytes(u0.at[pl.ds(0, 2), slab, grown], load_sem.at[0])
    take_row(u0, 0, 2)
    row_copies[0].start()

    @pl.loop(2, chunks)
    def _(k):
        sent(0, k).start()

    @pl.loop(0, chunks)
    def _(k):
        sent(1, k).start()

    beside_count = has[0].astype(jnp.int32) + has[1].astype(jnp.int32)

    @pl.when(host)
    def _():
        pl.semaphore_wait(barrier, beside_count)
        signal(met, partner)

    @pl.when(guest)
    def _():
        pl.semaphore_wait(met, 1)

    for side in (0, 1):

        @pl.when(jnp.logical_and(odd, has[side]))
        def _():
            signal(met, sides[side])

    @pl.when(jnp.logical_not(odd))
    def _():
        pl.semaphore_wait(met, beside_count)

    for side in (0, 1):

        @pl.when(has[side])
        def _():
            lab_copy(side).start()
            own_copy(side).start()

    @pl.loop(0, depth)
    def _(p):
        lab[p + 1, void_place] = jnp.full((EDGE, LANES), 3, jnp.int32)
        for place in range(4):
            u0[place, p + 1, void_place] = jnp.zeros((EDGE, LANES), jnp.float32)
            u1[place, p + 1, void_place] = jnp.zeros((EDGE, LANES), jnp.float32)

    for side in (0, 1):

        @pl.when(jnp.logical_not(has[side]))
        def _():
            plane = (0, depth + 1)[side]

            @pl.loop(0, chunks)
            def _(c):
                at = rows_of(c, EDGE)
                lab[plane, at] = jnp.full((CHUNK, LANES), 3, jnp.int32)
                for place in range(4):
                    u0[place, plane, at] = jnp.zeros((CHUNK, LANES), jnp.float32)
                    u1[place, plane, at] = jnp.zeros((CHUNK, LANES), jnp.float32)

    await_bytes(v, load_sem.at[2])
    row_copies[0].wait_recv()
    put_row(b0r, u0, 2, lambda j: 2 + j)

    await_bytes(u0.at[pl.ds(2, 2), slab, inner], in_recv.at[chunks])
    for side in (0, 1):

        @pl.when(has[side])
        def _():
            fwd_copy(side).start()

    await_sides(
        u1.at[0, pl.ds(0, 5), inner], u1.at[0, pl.ds(0, 10), inner], halo_recv.at[0]
    )

    await_bytes(lab.at[slab, grown], load_sem.at[1])

    @pl.loop(0, depth + 2)
    def _(p):
        @pl.loop(0, chunks)
        def _(c):
            at = rows_of(c, EDGE)
            cond[p, at] = label_values(lab[p, at], conductances, 0.0)

    @pl.loop(1, depth + 1)
    def _(p):
        for at in (pl.ds(0, EDGE), pl.ds(EDGE + rows, EDGE)):
            cond[p, at] = label_values(lab[p, at], conductances, 0.0)

    lane = lax.broadcasted_iota(jnp.int32, (STEP, LANES), 1)

    @pl.loop(0, depth)
    def _(p):
        @pl.loop(0, rows // STEP)
        def _(i):
            at, to = step_of(EDGE + STEP * i), step_of(STEP * i)
            row = EDGE + STEP * i
            center = cond[p + 1, at]
            beside = (
                cond[p + 2, at],
                cond[p, at],
                cond[p + 1, pl.ds(row + 1, STEP)],
                cond[p + 1, pl.ds(row - 1, STEP)],
                jnp.where(lane == LANES - 1, 0.0, pltpu.roll(center, LANES - 1, 1)),
                jnp.where(lane == 0, 0.0, pltpu.roll(center, 1, 1)),
            )
            total = jnp.zeros_like(center)
            for f in range(6):
                value = 2.0 * center * beside[f] / (center + beside[f])
                face[f, p, to] = value
                total = total + value
            face[6, p, to] = total
            exc[p, to] = label_values(lab[p + 1, at], excitability, 0.0)

    table = weight_table()
    weights = [
        [
            jnp.where(
                node == 0,
                jnp.float32(table[m][j]),
                jnp.float32(table[(m + 2) % 4][(j + 2) % 4]),
            )
            for j in range(4)
        ]
        for m in range(4)
    ]

    def sweep(source, start, steps, write):
        @pl.loop(0, depth * steps)
        def _(i):
            p, first = i % depth, start + STEP * (i // depth)
            at, to = step_of(EDGE + first), step_of(first)
            row = EDGE + first
            faces = [face[f, p, to] for f in range(7)]
            excite = exc[p, to]
            sum_u = [us[p, to]] * 4
            sum_v = [vs[p, to]] * 4
            for j in range(4):
                mid = source[j, p + 1, at]
                v_mid = v[j, p, to]
                spread = (
                    faces[0] * source[j, p + 2, at]
                    + faces[1] * source[j, p, at]
                    + faces[2] * source[j, p + 1, pl.ds(row + 1, STEP)]
                    + faces[3] * source[j, p + 1, pl.ds(row - 1, STEP)]
                    + faces[4] * pltpu.roll(mid, LANES - 1, 1)
                    + faces[5] * pltpu.roll(mid, 1, 1)
                )
                scaled = ionic_gain * mid
                growth = (scaled - ionic_gain * onset_level) * (1.0 - mid) - v_mid
                rate_u = spread + mid * (excite * growth - faces[6])
                recovery = recovery_base + recovery_slope * v_mid / jnp.maximum(
                    mid + recovery_offset, recovery_offset
                )
                rate_v = recovery * (-v_mid - scaled * (mid - (onset_level + 1.0)))
                for m in range(4):
                    sum_u[m] = sum_u[m] + weights[m][j] * rate_u
                    sum_v[m] = sum_v[m] + weights[m][j] * rate_v
            write(p, first, sum_u, sum_v)

    def first_sweep(k):
        def write(p, first, new_u, new_v):
            at, to = step_of(EDGE + first), step_of(first)
            for m in range(4):
                u1[m, p + 1, at] = new_u[m]
                v[m, p, to] = new_v[m]

        sweep(u0, CHUNK * mine(k), CHUNK // STEP, write)

    def second_sweep(row):
        def write(p, first, new_u, new_v):
            to, full = step_of(first), step_of(own + first)
            for m in range(2):
                out_u[m, p, full] = new_u[m]
                out_v[m, p, full] = new_v[m]
                res[m, p, to] = new_u[2 + m]
                v[2 + m, p, to] = new_v[2 + m]

        sweep(u1, row, 1, write)
        for copy in back_copies(row):
            copy.start()

    def await_mid(k):
        at = rows_of(mine(k), EDGE)
        await_sides(u1.at[:, pl.ds(0, 1), at], u1.at[:, pl.ds(0, 2), at], mid_recv.at[k])

    each = CHUNK // STEP
    steps = chunks * each

    @pl.loop(0, chunks + 1)
    def _(k):
        @pl.when(k < chunks)
        def _():
            arriving(1, k).wait_recv()
            first_sweep(k)
            for side in (0, 1):

                @pl.when(has[side])
                def _():
                    for pair in (0, 1):
                        mid_copy(side, pair, k).start()

        @pl.when(k == 0)
        def _():
            take_row(u1, 2, 4)
            row_copies[1].start()

        @pl.when(k == 1)
        def _():
            await_mid(0)

        @pl.when(jnp.logical_and(k > 0, k < chunks))
        def _():
            await_mid(k)

        @pl.when(k == chunks)
        def _():
            row_copies[1].wait_recv()
            put_row(b1r, u1, 4, lambda j: (j + 2) % 4)

        @pl.when(k > 0)
        def _():
            @pl.loop(0, each)
            def _(i):
                t = lax.rem(each * (k - 1) + 1 + i, steps)
                second_sweep(STEP * (t * half + (steps - 1 - t) * (1 - half)))

    await_sides(
        u1.at[0, pl.ds(0, 9), inner], u1.at[pl.ds(0, 2), pl.ds(0, 9), inner], side_send.at[0]
    )
    await_bytes(lines, row_send.at[0])
    await_bytes(v, in_send.at[0])
    await_bytes(v, back_send.at[0])
    await_bytes(v, back_recv.at[0])


def store(u_vmem, v_vmem, u_hbm, v_hbm, sem):
    pairs = ((u_vmem, u_hbm), (v_vmem, v_hbm))
    for i, (src, dst) in enumerate(pairs):
        for m in range(2):
            for p in range(u_vmem.shape[1]):
                pltpu.make_async_copy(src.at[m, p], dst.at[m, p], sem.at[i]).start()
    for i, (src, dst) in enumerate(pairs):
        pltpu.make_async_copy(src, dst, sem.at[i]).wait()


def on_device(*arguments):
    labels = arguments[2]
    depth, width = labels.shape[0], labels.shape[1]
    rows = width // 2
    chunks = rows // CHUNK
    tall = rows + 2 * EDGE
    f32 = jnp.float32
    hbm = pl.BlockSpec(memory_space=pltpu.HBM)
    vmem = pl.BlockSpec(memory_space=pltpu.VMEM)
    dma = pltpu.SemaphoreType.DMA
    result = jax.ShapeDtypeStruct((2, depth, width, LANES), f32)
    results = pl.pallas_call(
        kernel,
        out_shape=(result, result),
        in_specs=[hbm] * 5,
        out_specs=(vmem, vmem),
        scratch_shapes=[
            pltpu.VMEM((4, depth + 2, tall, LANES), f32),
            pltpu.VMEM((4, depth + 2, tall, LANES), f32),
            pltpu.VMEM((4, depth, rows, LANES), f32),
            pltpu.VMEM((2, depth, rows, LANES), f32),
            pltpu.VMEM((depth, rows, LANES), f32),
            pltpu.VMEM((depth, rows, LANES), f32),
            pltpu.VMEM((depth + 2, tall, LANES), jnp.int32),
            pltpu.VMEM((depth + 2, tall, LANES), f32),
            pltpu.VMEM((7, depth, rows, LANES), f32),
            pltpu.VMEM((depth, rows, LANES), f32),
            pltpu.VMEM((6, depth, LANES), f32),
            pltpu.VMEM((2, depth, LANES), f32),
            pltpu.VMEM((4, depth, LANES), f32),
            dma((3,)),
            dma((1,)),
            dma((1,)),
            dma((chunks,)),
            dma((1,)),
            dma((2,)),
            dma((1,)),
            dma((chunks + 1,)),
            dma((1,)),
            dma((1,)),
            pltpu.SemaphoreType.REGULAR,
            pltpu.SemaphoreType.REGULAR,
        ],
        compiler_params=pltpu.CompilerParams(
            collective_id=0, has_side_effects=True, vmem_limit_bytes=24 * 1024 * 1024
        ),
    )(*[pltpu.with_memory_space_constraint(x, pltpu.HBM) for x in arguments])
    return pl.pallas_call(
        store,
        out_shape=(result, result),
        in_specs=[vmem] * 2,
        out_specs=(hbm, hbm),
        scratch_shapes=[dma((2,))],
        compiler_params=pltpu.CompilerParams(vmem_limit_bytes=1024 * 1024),
    )(*results)


def solution(mesh):
    return jax.shard_map(
        on_device,
        mesh=mesh,
        in_specs=(
            P("space", None, None),
            P("space", None, None),
            P("space", None, None),
            P("node", "space", None, None),
            P("node", "space", None, None),
        ),
        out_specs=(P("node", "space", None, None), P("node", "space", None, None)),
        check_vma=False,
    )
```

```python
import jax
import jax.numpy as jnp
from jax import lax
from jax.experimental import pallas as pl
from jax.experimental.pallas import tpu as pltpu
from jax.sharding import PartitionSpec as P

MESH = pl.DeviceIdType.MESH
LANES = 128
CHUNK = 32
STEP = 16
EDGE = 8

radau_points = (0.08858795951270396, 0.4094668644407347, 0.7876594617608471, 1.0)
time_step = 0.16
onset_level = 0.15
ionic_gain = 8.0
recovery_base = 0.002
recovery_slope = 0.2
recovery_offset = 0.3
conductances = (1.0, 0.35, 0.05)
excitability = (1.0, 0.6, 0.0)


def weight_table():
    table = []
    for target in range(4):
        entries = []
        for column in range(4):
            coeffs = [1.0]
            for other in range(4):
                if other != column:
                    factor = 1.0 / (radau_points[column] - radau_points[other])
                    raised = [0.0] + coeffs
                    lowered = coeffs + [0.0]
                    coeffs = [
                        factor * (raised[place] - radau_points[other] * lowered[place])
                        for place in range(len(raised))
                    ]
            integral = 0.0
            for place in range(len(coeffs)):
                integral = integral + coeffs[place] * radau_points[target] ** (place + 1) / (
                    place + 1
                )
            entries.append(time_step * integral)
        table.append(entries)
    return table


def label_values(labels, values, outside):
    return jnp.where(
        labels == 0,
        jnp.float32(values[0]),
        jnp.where(
            labels == 1,
            jnp.float32(values[1]),
            jnp.where(labels == 2, jnp.float32(values[2]), jnp.float32(outside)),
        ),
    )


def kernel(
    us_hbm,
    vs_hbm,
    lab_hbm,
    ug_hbm,
    vg_hbm,
    out_u,
    out_v,
    u0,
    u1,
    v,
    res,
    us,
    vs,
    lab,
    cond,
    face,
    exc,
    lines,
    b0r,
    b1r,
    load_sem,
    side_send,
    halo_recv,
    mid_recv,
    row_send,
    row_recv,
    in_send,
    in_recv,
    back_send,
    back_recv,
    hello,
    met,
):
    depth, rows = lab_hbm.shape[0], lab_hbm.shape[1] // 2
    chunks = rows // CHUNK
    node, here = lax.axis_index("node"), lax.axis_index("space")
    count = lax.axis_size("space")
    fold = count // 2
    half = lax.rem(node + here // fold, 2)
    own, other = half * rows, (1 - half) * rows
    has = (here > 0, here < count - 1)
    flips = ((here == fold).astype(jnp.int32), (here == fold - 1).astype(jnp.int32))
    sides = (
        (lax.rem(node + flips[0], 2), here - 1),
        (lax.rem(node + flips[1], 2), here + 1),
    )
    partner = (1 - node, here)
    ours = (1, depth)
    theirs = (depth + 1, 0)

    def mine(k):
        return k * half + (chunks - 1 - k) * (1 - half)

    def its(k):
        return k * (1 - half) + (chunks - 1 - k) * half

    def rows_of(c, base):
        return pl.ds(pl.multiple_of(base + CHUNK * c, 8), CHUNK)

    def step_of(row):
        return pl.ds(pl.multiple_of(row, 8), STEP)

    def remote(src, dst, send, recv, device):
        return pltpu.make_async_remote_copy(
            src_ref=src,
            dst_ref=dst,
            send_sem=send,
            recv_sem=recv,
            device_id=device,
            device_id_type=MESH,
        )

    own_rows = pl.ds(pl.multiple_of(own, 8), rows)
    inner = pl.ds(EDGE, rows)
    slab = pl.ds(1, depth)
    edge_source = pl.ds(pl.multiple_of(rows - EDGE * half, 8), EDGE)
    edge_place = pl.ds(pl.multiple_of((EDGE + rows) * (1 - half), 8), EDGE)
    void_place = pl.ds(pl.multiple_of((EDGE + rows) * half, 8), EDGE)

    def lab_copy(side):
        return remote(
            lab_hbm.at[pl.ds(ours[side] - 1, 1), own_rows],
            lab.at[pl.ds(theirs[side], 1), inner],
            side_send.at[0],
            halo_recv.at[0],
            sides[side],
        )

    def own_copy(side):
        return remote(
            ug_hbm.at[:, pl.ds(ours[side] - 1, 1), own_rows],
            u0.at[pl.ds(2 * flips[side], 2), pl.ds(theirs[side], 1), inner],
            side_send.at[0],
            halo_recv.at[0],
            sides[side],
        )

    def fwd_copy(side):
        return remote(
            u0.at[pl.ds(2, 2), pl.ds(ours[side], 1), inner],
            u0.at[pl.ds(2 - 2 * flips[side], 2), pl.ds(theirs[side], 1), inner],
            side_send.at[0],
            halo_recv.at[0],
            sides[side],
        )

    def mid_copy(side, pair, k):
        at = rows_of(mine(k), EDGE)
        to = 2 * (pair + flips[side] - 2 * pair * flips[side])
        return remote(
            u1.at[pl.ds(2 * pair, 2), pl.ds(ours[side], 1), at],
            u1.at[pl.ds(to, 2), pl.ds(theirs[side], 1), at],
            side_send.at[0],
            mid_recv.at[k],
            sides[side],
        )

    def in_copy(field, k, c, base):
        return remote(
            (ug_hbm, vg_hbm)[field].at[:, :, rows_of(c, base)],
            (
                u0.at[pl.ds(2, 2), slab, rows_of(c, EDGE)],
                v.at[pl.ds(2, 2), :, rows_of(c, 0)],
            )[field],
            in_send.at[0],
            in_recv.at[k if field else chunks],
            partner,
        )

    def sent(field, k):
        return in_copy(field, k, its(k), other)

    def arriving(field, k):
        return in_copy(field, k, mine(k), own)

    def back_copies(row):
        to, full = step_of(row), step_of(own + row)
        return (
            remote(
                res.at[:, :, to],
                out_u.at[:, :, full],
                back_send.at[0],
                back_recv.at[0],
                partner,
            ),
            remote(
                v.at[pl.ds(2, 2), :, to],
                out_v.at[:, :, full],
                back_send.at[0],
                back_recv.at[0],
                partner,
            ),
        )

    row_copies = (
        remote(lines.at[pl.ds(0, 2)], b0r, row_send.at[0], row_recv.at[0], partner),
        remote(lines.at[pl.ds(2, 4)], b1r, row_send.at[0], row_recv.at[1], partner),
    )

    loads = [
        pltpu.make_async_copy(src, dst, load_sem.at[i])
        for i, src, dst in (
            (0, ug_hbm.at[:, :, own_rows], u0.at[pl.ds(0, 2), slab, inner]),
            (0, ug_hbm.at[:, :, edge_source], u0.at[pl.ds(0, 2), slab, edge_place]),
            (1, lab_hbm.at[:, own_rows], lab.at[slab, inner]),
            (1, lab_hbm.at[:, edge_source], lab.at[slab, edge_place]),
            (2, vg_hbm.at[:, :, own_rows], v.at[pl.ds(0, 2)]),
            (2, us_hbm.at[:, own_rows], us),
            (2, vs_hbm.at[:, own_rows], vs),
        )
    ]
    grown = pl.ds(pl.multiple_of(EDGE * (1 - half), 8), EDGE + rows)

    def await_bytes(ref, sem):
        pltpu.make_async_copy(ref, ref, sem).wait()

    both = jnp.logical_and(has[0], has[1])

    def await_sides(few, all_of_them, sem):
        @pl.when(both)
        def _():
            await_bytes(all_of_them, sem)

        @pl.when(jnp.logical_not(both))
        def _():
            await_bytes(few, sem)

    odd, first = here % 2 == 0, node == 1
    host = jnp.logical_and(odd, jnp.logical_not(first))
    guest = jnp.logical_and(odd, first)
    barrier = pltpu.get_barrier_semaphore()

    def signal(sem, device):
        pl.semaphore_signal(sem, inc=1, device_id=device, device_id_type=MESH)

    for copy in loads[:2]:
        copy.start()

    @pl.when(jnp.logical_not(guest))
    def _():
        signal(barrier, partner)

    @pl.when(jnp.logical_not(host))
    def _():
        pl.semaphore_wait(barrier, 1)

    @pl.when(guest)
    def _():
        signal(hello, partner)

    @pl.when(host)
    def _():
        pl.semaphore_wait(hello, 1)

    remote(
        ug_hbm.at[:, :, pl.ds(pl.multiple_of(other, 8), rows)],
        u0.at[pl.ds(2, 2), slab, inner],
        in_send.at[0],
        in_recv.at[chunks],
        partner,
    ).start()
    for copy in loads[2:]:
        copy.start()
    for side in (0, 1):

        @pl.when(jnp.logical_and(has[side], jnp.logical_not(jnp.logical_or(odd, sides[side][0] == 1))))
        def _():
            signal(barrier, sides[side])

    def take_row(source, place, nodes):
        line = EDGE + (rows - 1) * (1 - half)

        @pl.loop(0, depth)
        def _(p):
            for j in range(nodes):
                lines[place + j, pl.ds(p, 1)] = source[j, p + 1, pl.ds(line, 1)]

    def put_row(source, target, nodes, first):
        line = EDGE - 1 + (rows + 1) * (1 - half)

        @pl.loop(0, depth)
        def _(p):
            for j in range(nodes):
                target[first(j), p + 1, pl.ds(line, 1)] = source[j, pl.ds(p, 1)]

    await_bytes(u0.at[pl.ds(0, 2), slab, grown], load_sem.at[0])
    take_row(u0, 0, 2)
    row_copies[0].start()

    @pl.loop(0, chunks)
    def _(k):
        sent(1, k).start()

    beside_count = has[0].astype(jnp.int32) + has[1].astype(jnp.int32)

    @pl.when(host)
    def _():
        pl.semaphore_wait(barrier, beside_count)
        signal(met, partner)

    @pl.when(guest)
    def _():
        pl.semaphore_wait(met, 1)

    for side in (0, 1):

        @pl.when(jnp.logical_and(odd, has[side]))
        def _():
            signal(met, sides[side])

    @pl.when(jnp.logical_not(odd))
    def _():
        pl.semaphore_wait(met, beside_count)

    for side in (0, 1):

        @pl.when(has[side])
        def _():
            lab_copy(side).start()
            own_copy(side).start()

    @pl.loop(0, depth)
    def _(p):
        lab[p + 1, void_place] = jnp.full((EDGE, LANES), 3, jnp.int32)
        for place in range(4):
            u0[place, p + 1, void_place] = jnp.zeros((EDGE, LANES), jnp.float32)
            u1[place, p + 1, void_place] = jnp.zeros((EDGE, LANES), jnp.float32)

    for side in (0, 1):

        @pl.when(jnp.logical_not(has[side]))
        def _():
            plane = (0, depth + 1)[side]

            @pl.loop(0, chunks)
            def _(c):
                at = rows_of(c, EDGE)
                lab[plane, at] = jnp.full((CHUNK, LANES), 3, jnp.int32)
                for place in range(4):
                    u0[place, plane, at] = jnp.zeros((CHUNK, LANES), jnp.float32)
                    u1[place, plane, at] = jnp.zeros((CHUNK, LANES), jnp.float32)

    await_bytes(v, load_sem.at[2])
    row_copies[0].wait_recv()
    put_row(b0r, u0, 2, lambda j: 2 + j)

    await_bytes(u0.at[pl.ds(2, 2), slab, inner], in_recv.at[chunks])
    for side in (0, 1):

        @pl.when(has[side])
        def _():
            fwd_copy(side).start()

    await_sides(
        u1.at[0, pl.ds(0, 5), inner], u1.at[0, pl.ds(0, 10), inner], halo_recv.at[0]
    )

    await_bytes(lab.at[slab, grown], load_sem.at[1])

    @pl.loop(0, depth + 2)
    def _(p):
        @pl.loop(0, chunks)
        def _(c):
            at = rows_of(c, EDGE)
            cond[p, at] = label_values(lab[p, at], conductances, 0.0)

    @pl.loop(1, depth + 1)
    def _(p):
        for at in (pl.ds(0, EDGE), pl.ds(EDGE + rows, EDGE)):
            cond[p, at] = label_values(lab[p, at], conductances, 0.0)

    lane = lax.broadcasted_iota(jnp.int32, (STEP, LANES), 1)

    @pl.loop(0, depth)
    def _(p):
        @pl.loop(0, rows // STEP)
        def _(i):
            at, to = step_of(EDGE + STEP * i), step_of(STEP * i)
            row = EDGE + STEP * i
            center = cond[p + 1, at]
            beside = (
                cond[p + 2, at],
                cond[p, at],
                cond[p + 1, pl.ds(row + 1, STEP)],
                cond[p + 1, pl.ds(row - 1, STEP)],
                jnp.where(lane == LANES - 1, 0.0, pltpu.roll(center, LANES - 1, 1)),
                jnp.where(lane == 0, 0.0, pltpu.roll(center, 1, 1)),
            )
            total = jnp.zeros_like(center)
            for f in range(6):
                value = 2.0 * center * beside[f] / (center + beside[f])
                face[f, p, to] = value
                total = total + value
            face[6, p, to] = total
            exc[p, to] = label_values(lab[p + 1, at], excitability, 0.0)

    table = weight_table()
    weights = [
        [
            jnp.where(
                node == 0,
                jnp.float32(table[m][j]),
                jnp.float32(table[(m + 2) % 4][(j + 2) % 4]),
            )
            for j in range(4)
        ]
        for m in range(4)
    ]

    def sweep(source, start, steps, write):
        @pl.loop(0, depth * steps)
        def _(i):
            p, first = i % depth, start + STEP * (i // depth)
            at, to = step_of(EDGE + first), step_of(first)
            row = EDGE + first
            faces = [face[f, p, to] for f in range(7)]
            excite = exc[p, to]
            sum_u = [us[p, to]] * 4
            sum_v = [vs[p, to]] * 4
            for j in range(4):
                mid = source[j, p + 1, at]
                v_mid = v[j, p, to]
                spread = (
                    faces[0] * source[j, p + 2, at]
                    + faces[1] * source[j, p, at]
                    + faces[2] * source[j, p + 1, pl.ds(row + 1, STEP)]
                    + faces[3] * source[j, p + 1, pl.ds(row - 1, STEP)]
                    + faces[4] * pltpu.roll(mid, LANES - 1, 1)
                    + faces[5] * pltpu.roll(mid, 1, 1)
                )
                scaled = ionic_gain * mid
                growth = (scaled - ionic_gain * onset_level) * (1.0 - mid) - v_mid
                rate_u = spread + mid * (excite * growth - faces[6])
                recovery = recovery_base + recovery_slope * v_mid / jnp.maximum(
                    mid + recovery_offset, recovery_offset
                )
                rate_v = recovery * (-v_mid - scaled * (mid - (onset_level + 1.0)))
                for m in range(4):
                    sum_u[m] = sum_u[m] + weights[m][j] * rate_u
                    sum_v[m] = sum_v[m] + weights[m][j] * rate_v
            write(p, first, sum_u, sum_v)

    def first_sweep(k):
        def write(p, first, new_u, new_v):
            at, to = step_of(EDGE + first), step_of(first)
            for m in range(4):
                u1[m, p + 1, at] = new_u[m]
                v[m, p, to] = new_v[m]

        sweep(u0, CHUNK * mine(k), CHUNK // STEP, write)

    def second_sweep(row):
        def write(p, first, new_u, new_v):
            to, full = step_of(first), step_of(own + first)
            for m in range(2):
                out_u[m, p, full] = new_u[m]
                out_v[m, p, full] = new_v[m]
                res[m, p, to] = new_u[2 + m]
                v[2 + m, p, to] = new_v[2 + m]

        sweep(u1, row, 1, write)
        for copy in back_copies(row):
            copy.start()

    def await_mid(k):
        at = rows_of(mine(k), EDGE)
        await_sides(u1.at[:, pl.ds(0, 1), at], u1.at[:, pl.ds(0, 2), at], mid_recv.at[k])

    each = CHUNK // STEP
    steps = chunks * each

    @pl.loop(0, chunks + 1)
    def _(k):
        @pl.when(k < chunks)
        def _():
            arriving(1, k).wait_recv()
            first_sweep(k)
            for side in (0, 1):

                @pl.when(has[side])
                def _():
                    for pair in (0, 1):
                        mid_copy(side, pair, k).start()

        @pl.when(k == 0)
        def _():
            take_row(u1, 2, 4)
            row_copies[1].start()

        @pl.when(k == 1)
        def _():
            await_mid(0)

        @pl.when(jnp.logical_and(k > 0, k < chunks))
        def _():
            await_mid(k)

        @pl.when(k == chunks)
        def _():
            row_copies[1].wait_recv()
            put_row(b1r, u1, 4, lambda j: (j + 2) % 4)

        @pl.when(k > 0)
        def _():
            @pl.loop(0, each)
            def _(i):
                t = lax.rem(each * (k - 1) + 1 + i, steps)
                second_sweep(STEP * (t * half + (steps - 1 - t) * (1 - half)))

    await_sides(
        u1.at[0, pl.ds(0, 9), inner], u1.at[pl.ds(0, 2), pl.ds(0, 9), inner], side_send.at[0]
    )
    await_bytes(lines, row_send.at[0])
    await_bytes(v, in_send.at[0])
    await_bytes(v, back_send.at[0])
    await_bytes(v, back_recv.at[0])


def store(u_vmem, v_vmem, u_hbm, v_hbm, sem):
    pairs = ((u_vmem, u_hbm), (v_vmem, v_hbm))
    for i, (src, dst) in enumerate(pairs):
        for m in range(2):
            for p in range(u_vmem.shape[1]):
                pltpu.make_async_copy(src.at[m, p], dst.at[m, p], sem.at[i]).start()
    for i, (src, dst) in enumerate(pairs):
        pltpu.make_async_copy(src, dst, sem.at[i]).wait()


def on_device(*arguments):
    labels = arguments[2]
    depth, width = labels.shape[0], labels.shape[1]
    rows = width // 2
    chunks = rows // CHUNK
    tall = rows + 2 * EDGE
    f32 = jnp.float32
    hbm = pl.BlockSpec(memory_space=pltpu.HBM)
    vmem = pl.BlockSpec(memory_space=pltpu.VMEM)
    dma = pltpu.SemaphoreType.DMA
    result = jax.ShapeDtypeStruct((2, depth, width, LANES), f32)
    results = pl.pallas_call(
        kernel,
        out_shape=(result, result),
        in_specs=[hbm] * 5,
        out_specs=(vmem, vmem),
        scratch_shapes=[
            pltpu.VMEM((4, depth + 2, tall, LANES), f32),
            pltpu.VMEM((4, depth + 2, tall, LANES), f32),
            pltpu.VMEM((4, depth, rows, LANES), f32),
            pltpu.VMEM((2, depth, rows, LANES), f32),
            pltpu.VMEM((depth, rows, LANES), f32),
            pltpu.VMEM((depth, rows, LANES), f32),
            pltpu.VMEM((depth + 2, tall, LANES), jnp.int32),
            pltpu.VMEM((depth + 2, tall, LANES), f32),
            pltpu.VMEM((7, depth, rows, LANES), f32),
            pltpu.VMEM((depth, rows, LANES), f32),
            pltpu.VMEM((6, depth, LANES), f32),
            pltpu.VMEM((2, depth, LANES), f32),
            pltpu.VMEM((4, depth, LANES), f32),
            dma((3,)),
            dma((1,)),
            dma((1,)),
            dma((chunks,)),
            dma((1,)),
            dma((2,)),
            dma((1,)),
            dma((chunks + 1,)),
            dma((1,)),
            dma((1,)),
            pltpu.SemaphoreType.REGULAR,
            pltpu.SemaphoreType.REGULAR,
        ],
        compiler_params=pltpu.CompilerParams(
            collective_id=0, has_side_effects=True, vmem_limit_bytes=24 * 1024 * 1024
        ),
    )(*[pltpu.with_memory_space_constraint(x, pltpu.HBM) for x in arguments])
    return pl.pallas_call(
        store,
        out_shape=(result, result),
        in_specs=[vmem] * 2,
        out_specs=(hbm, hbm),
        scratch_shapes=[dma((2,))],
        compiler_params=pltpu.CompilerParams(vmem_limit_bytes=1024 * 1024),
    )(*results)


def solution(mesh):
    return jax.shard_map(
        on_device,
        mesh=mesh,
        in_specs=(
            P("space", None, None),
            P("space", None, None),
            P("space", None, None),
            P("node", "space", None, None),
            P("node", "space", None, None),
        ),
        out_specs=(P("node", "space", None, None), P("node", "space", None, None)),
        check_vma=False,
    )
```
